128 devices in a mesh: dp: 1, vp: 128 (over z, y, x, core).
Axes of the slice: x: 4, y: 4, z: 4, core: 2. Of those that a mesh axis runs over, the one named last changes fastest.
Arguments:
- hidden: bfloat16 [8192, 3584], P(('dp', 'vp'))
- target: int32 [8192], P('dp')
- norm_gain: bfloat16 [3584], replicated
- head_weight: bfloat16 [3584, 151936], P(None, 'vp')
Outputs:
- output 1: float32 [8192], P('dp')
- output 2: float32 [8192], P('dp')
- output 3: float32 [1], P('dp')
All inputs are finite; a program needn't handle non-finite values.
Results may differ from the reference program's by a relative error of at most 0.001.
Values are sent between devices in bfloat16 or wider.
A program may use at most 1 GiB of HBM per device.

```python
import math
import jax
import jax.numpy as jnp
from jax import lax

D = 3584
VOCAB = 151936
TOK_DEV = 64
GROUP = 128
HEAD_BLOCK = 128
NORM_EPS = 1e-6
TOKENS = TOK_DEV * GROUP
ROW_BLOCK = math.gcd(TOKENS, 64)


def setup_inputs(seed: int = 0, part: int = 0) -> dict:
    key = jax.random.key(seed)
    part_key = jax.random.fold_in(key, part)
    hidden_key, target_key = jax.random.split(part_key)
    gain_key, head_key = jax.random.split(jax.random.fold_in(key, 1000003))
    hidden = jax.random.normal(hidden_key, (TOKENS, D), jnp.float32).astype(jnp.bfloat16)
    target = jax.random.randint(target_key, (TOKENS,), 0, VOCAB, jnp.int32)
    target = target.at[0].set(0).at[TOKENS - 1].set(VOCAB - 1)
    norm_gain = (1.0 + 0.5 * jax.random.normal(gain_key, (D,), jnp.float32)).astype(jnp.bfloat16)
    head_scale = 1.5 / math.sqrt(D)

    def draw_rows(row_key):
        return (jax.random.normal(row_key, (HEAD_BLOCK, VOCAB), jnp.float32) * head_scale).astype(jnp.bfloat16)

    head_weight = lax.map(draw_rows, jax.random.split(head_key, D // HEAD_BLOCK)).reshape(D, VOCAB)
    return {"hidden": hidden, "target": target, "norm_gain": norm_gain, "head_weight": head_weight}


def reference(hidden, target, norm_gain, head_weight):
    hidden_f32 = hidden.astype(jnp.float32)
    inv_rms = lax.rsqrt(jnp.mean(hidden_f32 * hidden_f32, axis=-1, keepdims=True) + NORM_EPS)
    normed = (hidden_f32 * inv_rms * norm_gain.astype(jnp.float32)).astype(jnp.bfloat16)
    vocab_ids = jnp.arange(VOCAB, dtype=jnp.int32)

    def score_block(block_args):
        block_rows, block_target = block_args
        logits = jnp.dot(block_rows, head_weight, preferred_element_type=jnp.float32)
        row_max = jnp.max(logits, axis=-1, keepdims=True)
        shifted = logits - row_max
        exp_vals = jnp.exp(shifted)
        exp_total = jnp.sum(exp_vals, axis=-1)
        moment = jnp.sum(exp_vals * shifted, axis=-1)
        target_shift = jnp.sum(jnp.where(vocab_ids[None, :] == block_target[:, None], shifted, 0.0), axis=-1)
        log_total = jnp.log(exp_total)
        return target_shift - log_total, log_total - moment / exp_total

    num_blocks = TOKENS // ROW_BLOCK
    log_prob, entropy = lax.map(score_block, (normed.reshape(num_blocks, ROW_BLOCK, D), target.reshape(num_blocks, ROW_BLOCK)))
    log_prob = log_prob.reshape(TOKENS)
    entropy = entropy.reshape(TOKENS)
    return log_prob, entropy, jnp.mean(log_prob).reshape(1)
```

```python
import functools

import jax
import jax.numpy as jnp
from jax import lax
from jax.experimental import pallas as pl
from jax.experimental.pallas import tpu as pltpu
from jax.sharding import PartitionSpec as P

NORM_EPS = 1e-6
MESH = pl.DeviceIdType.MESH
SIDE = 4
CHIPS = SIDE**3
OWN = CHIPS - 1
LOW = -3.0e38
DIRS = ((1, 0, 0), (0, 1, 0), (0, 0, 1), (-1, 0, 0), (0, -1, 0), (0, 0, -1))
FULL = 10

TREE = (
    (0, 63, (1, 0, 0)), (1, 63, (0, 1, 0)), (2, 63, (0, 0, 1)), (3, 63, (3, 0, 0)), (4, 63, (0, 3, 0)), (5, 63, (0, 0, 3)),
    (0, 4, (1, 3, 0)), (1, 0, (1, 1, 0)), (2, 4, (0, 3, 1)), (3, 3, (2, 0, 0)), (4, 4, (0, 2, 0)), (5, 0, (1, 0, 3)),
    (0, 2, (1, 0, 1)), (1, 3, (3, 1, 0)), (2, 3, (3, 0, 1)), (3, 4, (3, 3, 0)), (4, 5, (0, 3, 3)), (5, 5, (0, 0, 2)),
    (0, 7, (2, 1, 0)), (1, 2, (0, 1, 1)), (2, 6, (1, 3, 1)), (3, 5, (3, 0, 3)), (4, 9, (2, 3, 0)), (5, 1, (0, 1, 3)),
    (0, 11, (2, 0, 3)), (1, 17, (0, 1, 2)), (2, 12, (1, 0, 2)), (3, 16, (3, 3, 3)), (4, 11, (1, 3, 3)), (5, 16, (0, 3, 2)),
    (0, 10, (1, 2, 0)), (1, 19, (0, 2, 1)), (2, 9, (2, 0, 1)), (3, 8, (3, 3, 1)), (4, 16, (0, 2, 3)), (5, 7, (1, 1, 3)),
    (0, 26, (2, 0, 2)), (1, 12, (1, 1, 1)), (2, 14, (3, 0, 2)), (3, 19, (3, 1, 1)), (4, 15, (3, 2, 0)), (5, 13, (3, 1, 3)),
    (0, 35, (2, 1, 3)), (1, 18, (2, 2, 0)), (2, 30, (1, 2, 1)), (3, 29, (3, 3, 2)), (4, 28, (1, 2, 3)), (5, 35, (1, 1, 2)),
    (0, 28, (2, 3, 3)), (1, 36, (2, 1, 2)), (2, 31, (0, 2, 2)), (3, 31, (3, 2, 1)), (4, 26, (1, 3, 2)), (5, 41, (3, 1, 2)),
    (0, 46, (2, 2, 3)), (1, 41, (3, 2, 3)), (2, 43, (2, 2, 1)), (3, 39, (2, 1, 1)), (4, 32, (2, 3, 1)), (5, 46, (1, 2, 2)),
    (0, 52, (2, 3, 2)), (1, 49, (2, 2, 2)), (2, 51, (3, 2, 2)),
)
HALVES = 2
EVENTS = HALVES * (FULL + 1)
AHEAD = 2


def pieces_of(event):
    slot = event // HALVES
    return range(6 * slot, min(6 * slot + 6, OWN))


def kernel(hidden_ref, gain_ref, target_ref, head_ref, lp_ref, ent_ref, mean_ref, x_ref, w_ref, z_ref, tgt_ref, pack_ref,
           mine_ref, stat_ref, res_ref, fin_ref, peer_ref, send_sem, recv_sem, w_sem, w_send, w_recv, stat_send, stat_recv,
           fin_send, fin_recv, peer_send, peer_recv):
    rows, depth = hidden_ref.shape
    half = rows // HALVES
    vocab = head_ref.shape[1]
    tiles = pl.cdiv(vocab, 128)
    part_rows = 6 * half
    me = lax.axis_index("vp")
    group = lax.axis_index("dp")
    core = lax.rem(me, 2)
    chip = me // 2
    coords = (lax.rem(chip, SIDE), lax.rem(chip // SIDE, SIDE), chip // (SIDE * SIDE))
    sign = 1 - 2 * core
    partner = me + sign

    def device(there):
        return (group, there)

    def chip_at(offset):
        c = [lax.rem(coords[i] + sign * offset[i] + 2 * SIDE, SIDE) for i in range(3)]
        return (c[2] * SIDE + c[1]) * SIDE + c[0]

    def same_core(offset):
        return chip_at(offset) * 2 + core

    neighbours = [same_core(d) for d in DIRS]

    def behind(piece):
        return chip_at([-o for o in TREE[piece][2]])

    barrier = pltpu.get_barrier_semaphore()
    for there in (*neighbours, partner):
        pl.semaphore_signal(barrier, inc=1, device_id=device(there), device_id_type=MESH)
    own_head = pltpu.make_async_copy(head_ref, w_ref.at[0], w_sem)
    own_head.start()

    h = hidden_ref[...].astype(jnp.float32)
    inv_rms = lax.rsqrt(jnp.mean(h * h, axis=-1, keepdims=True) + NORM_EPS)
    normed = (h * inv_rms * gain_ref[...].astype(jnp.float32)).astype(jnp.bfloat16)
    for c in range(HALVES):
        x_ref[c, OWN] = normed[c * half : (c + 1) * half]

    pl.semaphore_wait(barrier, 7)

    def piece_copy(event, piece):
        d, parent, _ = TREE[piece]
        c = event % HALVES
        return pltpu.make_async_remote_copy(
            src_ref=x_ref.at[c, parent],
            dst_ref=x_ref.at[c, piece],
            send_sem=send_sem.at[event],
            recv_sem=recv_sem.at[event],
            device_id=device(neighbours[d]),
            device_id_type=MESH,
        )

    def send_event(event):
        for piece in pieces_of(event):
            piece_copy(event, piece).start()

    def event_bytes(event, sem):
        ps = pieces_of(event)
        block = x_ref.at[event % HALVES, ps.start : ps.stop]
        return pltpu.make_async_copy(block, block, sem.at[event])

    def stat_copy(piece):
        return pltpu.make_async_remote_copy(
            src_ref=mine_ref.at[piece // 2],
            dst_ref=stat_ref.at[piece],
            send_sem=stat_send,
            recv_sem=stat_recv,
            device_id=device(behind(piece) * 2 + core),
            device_id_type=MESH,
        )

    def send_stats(slot):
        for piece in pieces_of(HALVES * slot):
            stat_copy(piece).start()

    for event in range(HALVES):
        send_event(event)
    head_copy = pltpu.make_async_remote_copy(
        src_ref=head_ref, dst_ref=w_ref.at[1], send_sem=w_send, recv_sem=w_recv, device_id=device(partner), device_id_type=MESH
    )
    head_copy.start()

    def comm(event):
        slot = event // HALVES
        ahead = event + AHEAD
        if 2 * HALVES <= ahead < EVENTS:
            send_event(ahead)
        event_bytes(event, recv_sem).wait()
        if slot == 0:
            send_event(event + HALVES)
            if event + AHEAD < 2 * HALVES and False:
                pass
        if event % HALVES == 1 and slot >= 2:
            send_stats(slot - 2)

    lanes = lax.broadcasted_iota(jnp.int32, (half, 128), 1).astype(jnp.float32)
    eye_row = lax.broadcasted_iota(jnp.int32, (half, 128), 0)
    eye_lane = lax.broadcasted_iota(jnp.int32, (half, 128), 1)

    def targets(piece, source):
        row = target_ref[pl.ds(source, 1), :].astype(jnp.float32)
        for c in range(HALVES):
            hit = eye_lane == eye_row + (core * rows + c * half)
            column = jnp.sum(jnp.where(hit, row, 0.0), axis=1, keepdims=True)
            tgt_ref[c, piece] = column - lanes

    for piece in range(OWN):
        targets(piece, behind(piece))
    targets(OWN, chip)

    comm(0)
    comm(1)
    own_head.wait()
    head_copy.wait_recv()

    base = [(me * vocab).astype(jnp.float32), (partner * vocab).astype(jnp.float32)]
    lane_ids = lax.broadcasted_iota(jnp.int32, (half, 128), 1)
    last_ok = lane_ids < vocab - (tiles - 1) * 128

    def logits(x, at):
        n = x.shape[0]
        for b in range(2):
            z_ref[pl.ds(at, n), b * tiles * 128 : b * tiles * 128 + vocab] = jnp.dot(
                x, w_ref[b], preferred_element_type=jnp.float32
            )

    def strip_stats(at, c, piece, pack_at):
        def tile(b, k):
            return z_ref[pl.ds(at, half), (b * tiles + k) * 128 : (b * tiles + k + 1) * 128]

        def masked(k, v, other):
            return jnp.where(last_ok, v, other) if k == tiles - 1 else v

        top = tile(0, 0)
        for b in range(2):
            for k in range(tiles):
                top = jnp.maximum(top, masked(k, tile(b, k), LOW))
        total = jnp.zeros_like(top)
        moment = jnp.zeros_like(top)
        picked = jnp.zeros_like(top)
        for b in range(2):
            where = tgt_ref[c, piece] - base[b]
            for k in range(tiles):
                z = tile(b, k)
                shifted = z - top
                e = jnp.exp(shifted)
                total += masked(k, e, 0.0)
                moment += masked(k, e * shifted, 0.0)
                hit = where == float(128 * k)
                if k == tiles - 1:
                    hit = hit & last_ok
                picked = jnp.where(hit, z, picked)
        row_top = jnp.max(top, axis=1, keepdims=True)
        drop = top - row_top
        scale = jnp.exp(drop)
        row_moment = jnp.sum((moment + total * drop) * scale, axis=1, keepdims=True)
        row_total = jnp.sum(total * scale, axis=1, keepdims=True)
        row_picked = jnp.sum(picked, axis=1, keepdims=True)
        packed = jnp.where(lane_ids == 0, row_top, jnp.where(lane_ids == 1, row_total, jnp.where(lane_ids == 2, row_moment, row_picked)))
        pack_ref[pack_at, pl.ds(c * half, half), :] = packed

    def flush(pairs, first_pair):
        for i in range(pairs):
            block = pack_ref[2 * i : 2 * i + 2].reshape(2 * rows, 128)
            mine_ref[first_pair + i] = block.T[0:4, :]

    def compute(part):
        slot, c = part // HALVES, lax.rem(part, HALVES)
        x = x_ref[c, pl.ds(6 * slot, 6)].reshape(part_rows, depth)
        logits(x, 0)

        def strip(d, carry):
            strip_stats(pl.multiple_of(d * half, half), c, 6 * slot + d, d)
            return carry

        lax.fori_loop(0, 6, strip, 0)

        @pl.when(c == 1)
        def _():
            flush(3, 3 * slot)

    def step(part, carry):
        compute(part)
        for event in range(2, EVENTS):
            pl.when(part + 2 == event)(functools.partial(comm, event))
        return carry

    lax.fori_loop(0, 2 * FULL, step, 0)
    send_stats(FULL - 1)

    last = jnp.concatenate([x_ref[c, OWN - 3 : OWN + 1].reshape(4 * half, depth) for c in range(HALVES)], axis=0)
    logits(last, 0)
    for c in range(HALVES):

        def strip(d, carry, c=c):
            strip_stats(pl.multiple_of((4 * c + d) * half, half), c, OWN - 3 + d, d)
            return carry

        lax.fori_loop(0, 4, strip, 0)
    flush(2, 3 * FULL)
    send_stats(FULL)
    stat_ref[OWN] = mine_ref[OWN // 2]

    arrived = stat_ref.at[0:OWN]
    pltpu.make_async_copy(arrived, arrived, stat_recv).wait()
    piece_id = lax.broadcasted_iota(jnp.int32, (CHIPS, 128), 0)
    lane = lax.broadcasted_iota(jnp.int32, (CHIPS, 128), 1)
    ok = lax.rem(piece_id, 2) == lane // rows

    def folded(v, op):
        return op(v, pltpu.roll(v, rows, 1))

    tops = jnp.where(ok, stat_ref[:, 0, :], LOW)
    top = jnp.max(tops, axis=0, keepdims=True)
    top = folded(top, jnp.maximum)
    drop = tops - top
    scale = jnp.exp(drop)
    totals = stat_ref[:, 1, :]
    total = folded(jnp.sum(jnp.where(ok, totals * scale, 0.0), axis=0, keepdims=True), jnp.add)
    moments = (stat_ref[:, 2, :] + totals * drop) * scale
    moment = folded(jnp.sum(jnp.where(ok, moments, 0.0), axis=0, keepdims=True), jnp.add)
    picked = folded(jnp.sum(jnp.where(ok, stat_ref[:, 3, :], 0.0), axis=0, keepdims=True), jnp.add)
    log_total = jnp.log(total)
    mine = lax.broadcasted_iota(jnp.int32, (1, 128), 1) // rows == core
    res_ref[0:1, :] = jnp.where(mine, picked - top - log_total, 0.0)
    res_ref[1:2, :] = jnp.where(mine, log_total - moment / total, 0.0)
    fin_ref[chip] = res_ref[...]

    def fin_copy(there):
        return pltpu.make_async_remote_copy(
            src_ref=res_ref,
            dst_ref=fin_ref.at[chip],
            send_sem=fin_send,
            recv_sem=fin_recv,
            device_id=device(there * 2 + core),
            device_id_type=MESH,
        )

    def tell(i, carry):
        fin_copy(lax.rem(chip + i, CHIPS)).start()
        return carry

    lax.fori_loop(1, CHIPS, tell, 0)
    others = fin_ref.at[0 : CHIPS - 1]
    pltpu.make_async_copy(others, others, fin_recv).wait()
    across = pltpu.make_async_remote_copy(
        src_ref=fin_ref, dst_ref=peer_ref, send_sem=peer_send, recv_sem=peer_recv, device_id=device(partner), device_id_type=MESH
    )
    across.start()
    across.wait_recv()
    log_prob = fin_ref[:, 0, :] + peer_ref[:, 0, :]
    lp_ref[...] = log_prob
    ent_ref[...] = fin_ref[:, 1, :] + peer_ref[:, 1, :]
    mean_ref[0] = jnp.sum(log_prob) * (1.0 / (CHIPS * 2 * rows))

    across.wait_send()
    pltpu.make_async_copy(others, others, fin_send).wait()
    pltpu.make_async_copy(arrived, arrived, stat_send).wait()
    head_copy.wait_send()
    for event in range(EVENTS):
        event_bytes(event, send_sem).wait()


def solution(mesh):
    def local_step(hidden, target, norm_gain, head_weight):
        rows, depth = hidden.shape
        vocab = head_weight.shape[1]
        tiles = pl.cdiv(vocab, 128)
        half = rows // HALVES
        vmem = pl.BlockSpec(memory_space=pltpu.VMEM)
        dma = pltpu.SemaphoreType.DMA
        lp, ent, mean = pl.pallas_call(
            kernel,
            name="head",
            out_shape=(
                jax.ShapeDtypeStruct((CHIPS, 2 * rows), jnp.float32),
                jax.ShapeDtypeStruct((CHIPS, 2 * rows), jnp.float32),
                jax.ShapeDtypeStruct((1,), jnp.float32),
            ),
            in_specs=[vmem, vmem, vmem, pl.BlockSpec(memory_space=pl.ANY)],
            out_specs=(vmem, vmem, pl.BlockSpec(memory_space=pltpu.SMEM)),
            scratch_shapes=[
                pltpu.VMEM((HALVES, CHIPS, half, depth), jnp.bfloat16),
                pltpu.VMEM((2, depth, vocab), jnp.bfloat16),
                pltpu.VMEM((8 * half, 2 * tiles * 128), jnp.float32),
                pltpu.VMEM((HALVES, CHIPS, half, 128), jnp.float32),
                pltpu.VMEM((6, rows, 128), jnp.float32),
                pltpu.VMEM((CHIPS // 2, 4, 128), jnp.float32),
                pltpu.VMEM((CHIPS, 4, 128), jnp.float32),
                pltpu.VMEM((2, 128), jnp.float32),
                pltpu.VMEM((CHIPS, 2, 128), jnp.float32),
                pltpu.VMEM((CHIPS, 2, 128), jnp.float32),
                dma((EVENTS,)), dma((EVENTS,)), dma, dma, dma, dma, dma, dma, dma, dma, dma,
            ],
            compiler_params=pltpu.CompilerParams(
                collective_id=0, has_side_effects=True, vmem_limit_bytes=66_000_000
            ),
        )(hidden, norm_gain.reshape(1, depth), target.reshape(CHIPS, 2 * rows), head_weight)
        return lp.reshape(-1), ent.reshape(-1), mean

    return jax.shard_map(local_step, mesh=mesh, in_specs=(P(("dp", "vp"), None), P("dp"), P(None), P(None, "vp")), out_specs=(P("dp"), P("dp"), P("dp")), check_vma=False)
```

```python
import functools

import jax
import jax.numpy as jnp
from jax import lax
from jax.experimental import pallas as pl
from jax.experimental.pallas import tpu as pltpu
from jax.sharding import PartitionSpec as P

NORM_EPS = 1e-6
MESH = pl.DeviceIdType.MESH
SIDE = 4
CHIPS = SIDE**3
OWN = CHIPS - 1
LOW = -3.0e38
DIRS = ((1, 0, 0), (0, 1, 0), (0, 0, 1), (-1, 0, 0), (0, -1, 0), (0, 0, -1))
FULL = 10

PARENT = (
    63, 63, 63, 63, 63, 63, 4, 0, 4, 3, 4, 0, 2, 3, 3, 4, 5, 5, 7, 2, 6, 5, 9, 1, 11, 17, 12, 16, 11, 16, 10, 19,
    9, 8, 16, 7, 26, 12, 14, 19, 15, 13, 35, 18, 30, 29, 28, 35, 28, 36, 31, 31, 26, 41, 46, 41, 43, 39, 32, 46, 52, 49, 51,
)
HALVES = 2
EVENTS = HALVES * (FULL + 1)
GROUPS = EVENTS
AHEAD = 4
STAGES = 4
WIDE = 512


def offsets():
    out = {OWN: (0, 0, 0)}
    for j, parent in enumerate(PARENT):
        out[j] = tuple((a + b) % SIDE for a, b in zip(out[parent], DIRS[j % 6]))
    return out


OFFSET = offsets()


def pieces_of(slot):
    return range(6 * slot, min(6 * slot + 6, OWN))


def place(piece, c):
    if piece == OWN:
        return GROUPS - 1, c
    if piece >= 6 * FULL:
        return HALVES * FULL, piece - 6 * FULL + 3 * c
    return HALVES * (piece // 6) + c, piece % 6


def kernel(hidden_ref, gain_ref, target_ref, head_ref, lp_ref, ent_ref, mean_ref, x_ref, w_ref, stage_ref, rest_ref, za_ref, zb_ref,
           tgt_ref, pack_ref, mine_ref, stat_ref, res_ref, fin_ref, peer_ref, send_sem, recv_sem, stage_sem, rest_sem, w_send, w_recv,
           stat_send, stat_recv, fin_send, fin_recv, peer_send, peer_recv):
    rows, depth = hidden_ref.shape
    half = rows // HALVES
    vocab = head_ref.shape[0]
    tiles = pl.cdiv(vocab, 128)
    width = tiles * 128
    me = lax.axis_index("vp")
    group = lax.axis_index("dp")
    core = lax.rem(me, 2)
    chip = me // 2
    coords = (lax.rem(chip, SIDE), lax.rem(chip // SIDE, SIDE), chip // (SIDE * SIDE))
    sign = 1 - 2 * core
    partner = me + sign

    def device(there):
        return (group, there)

    def chip_at(offset):
        c = [lax.rem(coords[i] + sign * offset[i] + 2 * SIDE, SIDE) for i in range(3)]
        return (c[2] * SIDE + c[1]) * SIDE + c[0]

    neighbours = [chip_at(d) * 2 + core for d in DIRS]

    def behind(piece):
        return chip_at([-o for o in OFFSET[piece]])

    barrier = pltpu.get_barrier_semaphore()
    for there in (*neighbours, partner):
        pl.semaphore_signal(barrier, inc=1, device_id=device(there), device_id_type=MESH)

    def stage_copy(n):
        return pltpu.make_async_copy(head_ref.at[128 * n : 128 * n + 128], stage_ref.at[n % STAGES], stage_sem.at[n % STAGES])

    whole = vocab // 128
    for n in range(STAGES):
        stage_copy(n).start()
    rest_copy = pltpu.make_async_copy(head_ref.at[128 * whole : vocab], rest_ref, rest_sem)
    rest_copy.start()

    h = hidden_ref[...].astype(jnp.float32)
    inv_rms = lax.rsqrt(jnp.mean(h * h, axis=-1, keepdims=True) + NORM_EPS)
    normed = (h * inv_rms * gain_ref[...].astype(jnp.float32)).astype(jnp.bfloat16)
    for c in range(HALVES):
        x_ref[GROUPS - 1, c] = normed[c * half : (c + 1) * half]

    pl.semaphore_wait(barrier, 7)

    def send_event(event):
        c = event % HALVES
        for piece in pieces_of(event // HALVES):
            pltpu.make_async_remote_copy(
                src_ref=x_ref.at[place(PARENT[piece], c)],
                dst_ref=x_ref.at[place(piece, c)],
                send_sem=send_sem.at[event],
                recv_sem=recv_sem.at[event],
                device_id=device(neighbours[piece % 6]),
                device_id_type=MESH,
            ).start()

    def wait_event(event, sem):
        ps = pieces_of(event // HALVES)
        g, d = place(ps.start, event % HALVES)
        block = x_ref.at[g, d : d + len(ps)]
        pltpu.make_async_copy(block, block, sem.at[event]).wait()

    for event in range(HALVES):
        send_event(event)

    def head_copy(n):
        return pltpu.make_async_remote_copy(
            src_ref=w_ref.at[:, 128 * n : 128 * n + 128],
            dst_ref=w_ref.at[:, width + 128 * n : width + 128 * n + 128],
            send_sem=w_send,
            recv_sem=w_recv,
            device_id=device(partner),
            device_id_type=MESH,
        )

    for n in range(tiles):
        if n < whole:
            stage_copy(n).wait()
        else:
            rest_copy.wait()
            stage_ref[n % STAGES, 0 : vocab - 128 * whole] = rest_ref[...]

        def turn(k, carry, n=n):
            for u in range(4):
                at = pl.multiple_of((4 * k + u) * 128, 128)
                w_ref[pl.ds(at, 128), 128 * n : 128 * n + 128] = stage_ref[n % STAGES, :, pl.ds(at, 128)].T
            return carry

        lax.fori_loop(0, depth // 512, turn, 0)
        if n + STAGES < whole:
            stage_copy(n + STAGES).start()
        if n:
            head_copy(n - 1).start()

    lane_ids = lax.broadcasted_iota(jnp.int32, (half, 128), 1)
    row_ids = lax.broadcasted_iota(jnp.int32, (half, 128), 0)
    lanes = lane_ids.astype(jnp.float32)
    last_ok = lane_ids < vocab - (tiles - 1) * 128

    def targets(piece):
        row = target_ref[pl.ds(behind(piece), 1), :].astype(jnp.float32)
        for c in range(HALVES):
            hit = lane_ids == row_ids + (core * rows + c * half)
            column = jnp.sum(jnp.where(hit, row, 0.0), axis=1, keepdims=True)
            tgt_ref[place(piece, c)] = column - lanes

    for piece in range(CHIPS):
        targets(piece)
        if piece == 0:
            head_copy(tiles - 1).start()

    def comm(event):
        wait_event(event, recv_sem)
        if event < HALVES:
            send_event(event + HALVES)
        if event + AHEAD < EVENTS:
            send_event(event + AHEAD)

    comm(0)
    comm(1)
    partner_head = w_ref.at[:, width : 2 * width]
    pltpu.make_async_copy(partner_head, partner_head, w_recv).wait()

    base = [(me * vocab).astype(jnp.float32), (partner * vocab).astype(jnp.float32)]

    def strip_stats(z_ref, g, d, pack_at):
        def tile(b, k):
            return z_ref[d * half : (d + 1) * half, (b * tiles + k) * 128 : (b * tiles + k + 1) * 128]

        def masked(k, v, other):
            return jnp.where(last_ok, v, other) if k == tiles - 1 else v

        top = tile(0, 0)
        for b in range(2):
            for k in range(tiles):
                top = jnp.maximum(top, masked(k, tile(b, k), LOW))
        total = jnp.zeros_like(top)
        moment = jnp.zeros_like(top)
        picked = jnp.zeros_like(top)
        for b in range(2):
            where = tgt_ref[g, d] - base[b]
            for k in range(tiles):
                z = tile(b, k)
                shifted = z - top
                e = jnp.exp(shifted)
                total += masked(k, e, 0.0)
                moment += masked(k, e * shifted, 0.0)
                hit = where == float(128 * k)
                if k == tiles - 1:
                    hit = hit & last_ok
                picked = jnp.where(hit, z, picked)
        row_top = jnp.max(top, axis=1, keepdims=True)
        drop = top - row_top
        scale = jnp.exp(drop)
        row_moment = jnp.sum((moment + total * drop) * scale, axis=1, keepdims=True)
        row_total = jnp.sum(total * scale, axis=1, keepdims=True)
        row_picked = jnp.sum(picked, axis=1, keepdims=True)
        packed = jnp.where(lane_ids == 0, row_top, jnp.where(lane_ids == 1, row_total, jnp.where(lane_ids == 2, row_moment, row_picked)))
        pack_ref[pack_at] = packed

    def part(g, z_ref, before, other_ref, pack_at):
        x = x_ref[g].reshape(6 * half, depth)
        for n in range(2 * width // WIDE):
            at = slice(n * WIDE, (n + 1) * WIDE)
            z_ref[:, at] = jnp.dot(x, w_ref[:, at], preferred_element_type=jnp.float32)
            strip_stats(other_ref, before, n, pack_at(n))
        for d in range(2 * width // WIDE, 6):
            strip_stats(other_ref, before, d, pack_at(d))

    def flush(pairs, first_pair):
        for i in range(pairs):
            block = pack_ref[4 * i : 4 * i + 4].reshape(2 * rows, 128)
            mine_ref[first_pair + i] = block.T[0:4, :]

    def stat_copy(piece):
        return pltpu.make_async_remote_copy(
            src_ref=mine_ref.at[piece // 2],
            dst_ref=stat_ref.at[piece],
            send_sem=stat_send,
            recv_sem=stat_recv,
            device_id=device(behind(piece) * 2 + core),
            device_id_type=MESH,
        )

    def send_stats(slot):
        for piece in pieces_of(slot):
            stat_copy(piece).start()

    def at_turn(turn, first, last, what):
        for t in range(first, last):
            pl.when(turn == t)(functools.partial(what, t))

    def step(turn, carry):
        def before_first(t):
            comm(2 * t - 1)

        def before_second(t):
            comm(2 * t)
            if t == FULL:
                comm(2 * t + 1)
            if t >= 2:
                send_stats(t - 2)

        at_turn(turn, 2, FULL + 1, before_first)
        first = jnp.where(turn == 0, GROUPS - 1, 2 * turn - 1)
        part(first, za_ref, jnp.maximum(2 * turn - 2, 0), zb_ref, lambda d: 2 * d)
        at_turn(turn, 1, FULL + 1, before_second)
        part(2 * turn, zb_ref, first, za_ref, lambda d: jnp.where(turn == 0, d, 2 * d + 1))

        @pl.when(turn > 0)
        def _():
            flush(3, 3 * (turn - 1))

        @pl.when(turn == 0)
        def _():
            pack_ref[2] = pack_ref[0]
            pack_ref[3] = pack_ref[1]
            flush(1, OWN // 2)
            stat_ref[OWN] = mine_ref[OWN // 2]

        return carry

    lax.fori_loop(0, FULL + 1, step, 0)
    send_stats(FULL - 1)
    for d in range(6):
        strip_stats(zb_ref, HALVES * FULL, d, 2 * (d % 3) + d // 3)
    flush(2, 3 * FULL)
    send_stats(FULL)

    arrived = stat_ref.at[0:OWN]
    pltpu.make_async_copy(arrived, arrived, stat_recv).wait()
    piece_id = lax.broadcasted_iota(jnp.int32, (CHIPS, 128), 0)
    lane = lax.broadcasted_iota(jnp.int32, (CHIPS, 128), 1)
    ok = lax.rem(piece_id, 2) == lane // rows

    def folded(v, op):
        return op(v, pltpu.roll(v, rows, 1))

    tops = jnp.where(ok, stat_ref[:, 0, :], LOW)
    top = jnp.max(tops, axis=0, keepdims=True)
    top = folded(top, jnp.maximum)
    drop = tops - top
    scale = jnp.exp(drop)
    totals = stat_ref[:, 1, :]
    total = folded(jnp.sum(jnp.where(ok, totals * scale, 0.0), axis=0, keepdims=True), jnp.add)
    moments = (stat_ref[:, 2, :] + totals * drop) * scale
    moment = folded(jnp.sum(jnp.where(ok, moments, 0.0), axis=0, keepdims=True), jnp.add)
    picked = folded(jnp.sum(jnp.where(ok, stat_ref[:, 3, :], 0.0), axis=0, keepdims=True), jnp.add)
    log_total = jnp.log(total)
    mine = lax.broadcasted_iota(jnp.int32, (1, 128), 1) // rows == core
    res_ref[0:1, :] = jnp.where(mine, picked - top - log_total, 0.0)
    res_ref[1:2, :] = jnp.where(mine, log_total - moment / total, 0.0)
    fin_ref[chip] = res_ref[...]

    def fin_copy(there):
        return pltpu.make_async_remote_copy(
            src_ref=res_ref,
            dst_ref=fin_ref.at[chip],
            send_sem=fin_send,
            recv_sem=fin_recv,
            device_id=device(there * 2 + core),
            device_id_type=MESH,
        )

    def tell(i, carry):
        fin_copy(lax.rem(chip + i, CHIPS)).start()
        return carry

    lax.fori_loop(1, CHIPS, tell, 0)
    others = fin_ref.at[0 : CHIPS - 1]
    pltpu.make_async_copy(others, others, fin_recv).wait()
    across = pltpu.make_async_remote_copy(
        src_ref=fin_ref, dst_ref=peer_ref, send_sem=peer_send, recv_sem=peer_recv, device_id=device(partner), device_id_type=MESH
    )
    across.start()
    across.wait_recv()
    log_prob = fin_ref[:, 0, :] + peer_ref[:, 0, :]
    lp_ref[...] = log_prob
    ent_ref[...] = fin_ref[:, 1, :] + peer_ref[:, 1, :]
    mean_ref[0] = jnp.sum(log_prob) * (1.0 / (CHIPS * 2 * rows))

    across.wait_send()
    pltpu.make_async_copy(others, others, fin_send).wait()
    pltpu.make_async_copy(arrived, arrived, stat_send).wait()
    pltpu.make_async_copy(partner_head, partner_head, w_send).wait()
    for event in range(EVENTS):
        wait_event(event, send_sem)


def solution(mesh):
    def local_step(hidden, target, norm_gain, head_weight):
        rows, depth = hidden.shape
        vocab = head_weight.shape[1]
        width = pl.cdiv(vocab, 128) * 128
        half = rows // HALVES
        vmem = pl.BlockSpec(memory_space=pltpu.VMEM)
        dma = pltpu.SemaphoreType.DMA
        lp, ent, mean = pl.pallas_call(
            kernel,
            name="head",
            out_shape=(
                jax.ShapeDtypeStruct((CHIPS, 2 * rows), jnp.float32),
                jax.ShapeDtypeStruct((CHIPS, 2 * rows), jnp.float32),
                jax.ShapeDtypeStruct((1,), jnp.float32),
            ),
            in_specs=[vmem, vmem, vmem, pl.BlockSpec(memory_space=pl.ANY)],
            out_specs=(vmem, vmem, pl.BlockSpec(memory_space=pltpu.SMEM)),
            scratch_shapes=[
                pltpu.VMEM((GROUPS, 6, half, depth), jnp.bfloat16),
                pltpu.VMEM((depth, 2 * width), jnp.bfloat16),
                pltpu.VMEM((STAGES, 128, depth), jnp.bfloat16),
                pltpu.VMEM((vocab % 128, depth), jnp.bfloat16),
                pltpu.VMEM((6 * half, 2 * width), jnp.float32),
                pltpu.VMEM((6 * half, 2 * width), jnp.float32),
                pltpu.VMEM((GROUPS, 6, half, 128), jnp.float32),
                pltpu.VMEM((12, half, 128), jnp.float32),
                pltpu.VMEM((CHIPS // 2, 4, 128), jnp.float32),
                pltpu.VMEM((CHIPS, 4, 128), jnp.float32),
                pltpu.VMEM((2, 128), jnp.float32),
                pltpu.VMEM((CHIPS, 2, 128), jnp.float32),
                pltpu.VMEM((CHIPS, 2, 128), jnp.float32),
                dma((EVENTS,)), dma((EVENTS,)), dma((STAGES,)), dma, dma, dma, dma, dma, dma, dma, dma, dma,
            ],
            compiler_params=pltpu.CompilerParams(
                collective_id=0, has_side_effects=True, vmem_limit_bytes=67_000_000
            ),
        )(hidden, norm_gain, target.reshape(CHIPS, 2 * rows), head_weight.T)
        return lp.reshape(-1), ent.reshape(-1), mean

    return jax.shard_map(local_step, mesh=mesh, in_specs=(P(("dp", "vp"), None), P("dp"), P(None), P(None, "vp")), out_specs=(P("dp"), P("dp"), P("dp")), check_vma=False)
```

```python
import functools
import itertools

import jax
import jax.numpy as jnp
from jax import lax
from jax.experimental import pallas as pl
from jax.experimental.pallas import tpu as pltpu
from jax.sharding import PartitionSpec as P

NORM_EPS = 1e-6
MESH = pl.DeviceIdType.MESH
SIDE = 4
CHIPS = SIDE**3
OWN = CHIPS - 1
LOW = -3.0e38
DIRS = ((1, 0, 0), (0, 1, 0), (0, 0, 1), (-1, 0, 0), (0, -1, 0), (0, 0, -1))
FULL = 10

PARENT = (
    63, 63, 63, 63, 63, 63, 4, 0, 4, 3, 4, 0, 2, 3, 3, 4, 5, 5, 7, 2, 6, 5, 9, 1, 11, 17, 12, 16, 11, 16, 10, 19,
    9, 8, 16, 7, 26, 12, 14, 19, 15, 13, 35, 18, 30, 29, 28, 35, 28, 36, 31, 31, 26, 41, 46, 41, 43, 39, 32, 46, 52, 49, 51,
)
HALVES = 2
EVENTS = HALVES * (FULL + 1)
GROUPS = EVENTS
AHEAD = 4
STAGES = 4
WIDE = 512


def offsets():
    out = {OWN: (0, 0, 0)}
    for j, parent in enumerate(PARENT):
        out[j] = tuple((a + b) % SIDE for a, b in zip(out[parent], DIRS[j % 6]))
    return out


OFFSET = offsets()
FARTHEST = (SIDE // 2,) * 3


def pieces_of(slot):
    return range(6 * slot, min(6 * slot + 6, OWN))


def place(piece, c):
    if piece == OWN:
        return GROUPS - 1, c
    if piece >= 6 * FULL:
        return HALVES * FULL, piece - 6 * FULL + 3 * c
    return HALVES * (piece // 6) + c, piece % 6


def kernel(hidden_ref, gain_ref, target_ref, head_ref, out_ref, mean_ref, x_ref, w_ref, stage_ref, rest_ref, za_ref, zb_ref,
           tgt_ref, pack_ref, mine_ref, stat_ref, res_ref, fin_ref, send_sem, recv_sem, stage_sem, rest_sem, w_send, w_recv,
           stat_send, stat_recv, fin_send, fin_recv):
    rows, depth = hidden_ref.shape
    half = rows // HALVES
    vocab = head_ref.shape[0]
    tiles = pl.cdiv(vocab, 128)
    width = tiles * 128
    me = lax.axis_index("vp")
    group = lax.axis_index("dp")
    core = lax.rem(me, 2)
    chip = me // 2
    coords = (lax.rem(chip, SIDE), lax.rem(chip // SIDE, SIDE), chip // (SIDE * SIDE))
    sign = 1 - 2 * core
    partner = me + sign

    def device(there):
        return (group, there)

    def chip_at(offset):
        c = [lax.rem(coords[i] + sign * offset[i] + 2 * SIDE, SIDE) for i in range(3)]
        return (c[2] * SIDE + c[1]) * SIDE + c[0]

    neighbours = [chip_at(d) * 2 + core for d in DIRS]

    def behind(piece):
        return chip_at([-o for o in OFFSET[piece]])

    def merger(piece):
        return chip_at([SIDE // 2 - o for o in OFFSET[piece]])

    barrier = pltpu.get_barrier_semaphore()
    for there in (*neighbours, partner):
        pl.semaphore_signal(barrier, inc=1, device_id=device(there), device_id_type=MESH)

    def stage_copy(n):
        return pltpu.make_async_copy(head_ref.at[128 * n : 128 * n + 128], stage_ref.at[n % STAGES], stage_sem.at[n % STAGES])

    whole = vocab // 128
    for n in range(STAGES):
        stage_copy(n).start()
    rest_copy = pltpu.make_async_copy(head_ref.at[128 * whole : vocab], rest_ref, rest_sem)
    rest_copy.start()

    h = hidden_ref[...].astype(jnp.float32)
    inv_rms = lax.rsqrt(jnp.mean(h * h, axis=-1, keepdims=True) + NORM_EPS)
    normed = (h * inv_rms * gain_ref[...].astype(jnp.float32)).astype(jnp.bfloat16)
    for c in range(HALVES):
        x_ref[GROUPS - 1, c] = normed[c * half : (c + 1) * half]

    pl.semaphore_wait(barrier, 7)

    def send_event(event):
        c = event % HALVES
        for piece in pieces_of(event // HALVES):
            pltpu.make_async_remote_copy(
                src_ref=x_ref.at[place(PARENT[piece], c)],
                dst_ref=x_ref.at[place(piece, c)],
                send_sem=send_sem.at[event],
                recv_sem=recv_sem.at[event],
                device_id=device(neighbours[piece % 6]),
                device_id_type=MESH,
            ).start()

    def wait_event(event, sem):
        ps = pieces_of(event // HALVES)
        g, d = place(ps.start, event % HALVES)
        block = x_ref.at[g, d : d + len(ps)]
        pltpu.make_async_copy(block, block, sem.at[event]).wait()

    for event in range(HALVES):
        send_event(event)

    def head_copy(n):
        return pltpu.make_async_remote_copy(
            src_ref=w_ref.at[:, 128 * n : 128 * n + 128],
            dst_ref=w_ref.at[:, width + 128 * n : width + 128 * n + 128],
            send_sem=w_send,
            recv_sem=w_recv,
            device_id=device(partner),
            device_id_type=MESH,
        )

    for n in range(tiles):
        if n < whole:
            stage_copy(n).wait()
        else:
            rest_copy.wait()
            stage_ref[n % STAGES, 0 : vocab - 128 * whole] = rest_ref[...]

        def turn(k, carry, n=n):
            for u in range(4):
                at = pl.multiple_of((4 * k + u) * 128, 128)
                w_ref[pl.ds(at, 128), 128 * n : 128 * n + 128] = stage_ref[n % STAGES, :, pl.ds(at, 128)].T
            return carry

        lax.fori_loop(0, depth // 512, turn, 0)
        if n + STAGES < whole:
            stage_copy(n + STAGES).start()
        if n:
            head_copy(n - 1).start()

    lane_ids = lax.broadcasted_iota(jnp.int32, (half, 128), 1)
    row_ids = lax.broadcasted_iota(jnp.int32, (half, 128), 0)
    lanes = lane_ids.astype(jnp.float32)
    last_ok = lane_ids < vocab - (tiles - 1) * 128

    def targets(piece):
        row = target_ref[pl.ds(behind(piece), 1), :].astype(jnp.float32)
        for c in range(HALVES):
            hit = lane_ids == row_ids + (core * rows + c * half)
            column = jnp.sum(jnp.where(hit, row, 0.0), axis=1, keepdims=True)
            tgt_ref[place(piece, c)] = column - lanes

    for piece in range(CHIPS):
        targets(piece)
        if piece == 0:
            head_copy(tiles - 1).start()

    def comm(event):
        wait_event(event, recv_sem)
        if event < HALVES:
            send_event(event + HALVES)
        if event + AHEAD < EVENTS:
            send_event(event + AHEAD)

    comm(0)
    comm(1)
    partner_head = w_ref.at[:, width : 2 * width]
    pltpu.make_async_copy(partner_head, partner_head, w_recv).wait()

    base = [(me * vocab).astype(jnp.float32), (partner * vocab).astype(jnp.float32)]

    def strip_stats(z_ref, g, d, pack_at):
        def tile(b, k):
            return z_ref[d * half : (d + 1) * half, (b * tiles + k) * 128 : (b * tiles + k + 1) * 128]

        def masked(k, v, other):
            return jnp.where(last_ok, v, other) if k == tiles - 1 else v

        top = tile(0, 0)
        for b in range(2):
            for k in range(tiles):
                top = jnp.maximum(top, masked(k, tile(b, k), LOW))
        total = jnp.zeros_like(top)
        moment = jnp.zeros_like(top)
        picked = jnp.zeros_like(top)
        for b in range(2):
            where = tgt_ref[g, d] - base[b]
            for k in range(tiles):
                z = tile(b, k)
                shifted = z - top
                e = jnp.exp(shifted)
                total += masked(k, e, 0.0)
                moment += masked(k, e * shifted, 0.0)
                hit = where == float(128 * k)
                if k == tiles - 1:
                    hit = hit & last_ok
                picked = jnp.where(hit, z, picked)
        row_top = jnp.max(top, axis=1, keepdims=True)
        drop = top - row_top
        scale = jnp.exp(drop)
        row_moment = jnp.sum((moment + total * drop) * scale, axis=1, keepdims=True)
        row_total = jnp.sum(total * scale, axis=1, keepdims=True)
        row_picked = jnp.sum(picked, axis=1, keepdims=True)
        packed = jnp.where(lane_ids == 0, row_top, jnp.where(lane_ids == 1, row_total, jnp.where(lane_ids == 2, row_moment, row_picked)))
        pack_ref[pack_at] = packed

    def part(g, z_ref, before, other_ref, pack_at):
        x = x_ref[g].reshape(6 * half, depth)
        for n in range(2 * width // WIDE):
            at = slice(n * WIDE, (n + 1) * WIDE)
            z_ref[:, at] = jnp.dot(x, w_ref[:, at], preferred_element_type=jnp.float32)
            strip_stats(other_ref, before, n, pack_at(n))
        for d in range(2 * width // WIDE, 6):
            strip_stats(other_ref, before, d, pack_at(d))

    def flush(pairs, first_pair):
        for i in range(pairs):
            block = pack_ref[4 * i : 4 * i + 4].reshape(2 * rows, 128)
            mine_ref[first_pair + i] = block.T[0:4, :]

    def stat_copy(piece):
        return pltpu.make_async_remote_copy(
            src_ref=mine_ref.at[CHIPS // 2 if piece == OWN else piece // 2],
            dst_ref=stat_ref.at[piece],
            send_sem=stat_send,
            recv_sem=stat_recv,
            device_id=device(merger(piece) * 2 + core),
            device_id_type=MESH,
        )

    def send_stats(pieces):
        for piece in pieces:
            if OFFSET[piece] == FARTHEST:
                stat_ref[piece] = mine_ref[piece // 2]
            else:
                stat_copy(piece).start()

    def at_turn(turn, first, last, what):
        for t in range(first, last):
            pl.when(turn == t)(functools.partial(what, t))

    def step(turn, carry):
        def before_first(t):
            comm(2 * t - 1)

        def before_second(t):
            comm(2 * t)
            if t == FULL:
                comm(2 * t + 1)
            if t == FULL - 2:
                send_stats([*range(18), OWN])
            if t == FULL - 1:
                send_stats(range(18, 42))
            if t == FULL:
                send_stats(range(42, 54))

        at_turn(turn, 2, FULL + 1, before_first)
        first = jnp.where(turn == 0, GROUPS - 1, 2 * turn - 1)
        part(first, za_ref, jnp.maximum(2 * turn - 2, 0), zb_ref, lambda d: 2 * d)
        at_turn(turn, 1, FULL + 1, before_second)
        part(2 * turn, zb_ref, first, za_ref, lambda d: jnp.where(turn == 0, d, 2 * d + 1))

        @pl.when(turn > 0)
        def _():
            flush(3, 3 * (turn - 1))

        @pl.when(turn == 0)
        def _():
            pack_ref[2] = pack_ref[0]
            pack_ref[3] = pack_ref[1]
            flush(1, CHIPS // 2)

        return carry

    lax.fori_loop(0, FULL + 1, step, 0)
    send_stats(pieces_of(FULL - 1))
    for d in range(6):
        strip_stats(zb_ref, HALVES * FULL, d, 2 * (d % 3) + d // 3)
    flush(2, 3 * FULL)
    send_stats(pieces_of(FULL))

    arrived = stat_ref.at[0 : CHIPS - 1]
    pltpu.make_async_copy(arrived, arrived, stat_recv).wait()
    piece_id = lax.broadcasted_iota(jnp.int32, (CHIPS, 128), 0)
    lane = lax.broadcasted_iota(jnp.int32, (CHIPS, 128), 1)
    ok = lax.rem(piece_id, 2) == lane // rows

    def folded(v, op):
        return op(v, pltpu.roll(v, rows, 1))

    tops = jnp.where(ok, stat_ref[:, 0, :], LOW)
    top = jnp.max(tops, axis=0, keepdims=True)
    top = folded(top, jnp.maximum)
    drop = tops - top
    scale = jnp.exp(drop)
    totals = stat_ref[:, 1, :]
    total = folded(jnp.sum(jnp.where(ok, totals * scale, 0.0), axis=0, keepdims=True), jnp.add)
    moments = (stat_ref[:, 2, :] + totals * drop) * scale
    moment = folded(jnp.sum(jnp.where(ok, moments, 0.0), axis=0, keepdims=True), jnp.add)
    picked = folded(jnp.sum(jnp.where(ok, stat_ref[:, 3, :], 0.0), axis=0, keepdims=True), jnp.add)
    log_total = jnp.log(total)
    mine = lax.broadcasted_iota(jnp.int32, (1, 128), 1) // rows == core
    res_ref[0:1, :] = jnp.where(mine, picked - top - log_total, 0.0)
    res_ref[1:2, :] = jnp.where(mine, log_total - moment / total, 0.0)

    origin = core * CHIPS + merger(OWN)
    fin_ref[origin] = res_ref[...]
    steps = [[lax.rem(coords[i] + k, SIDE) for k in range(SIDE)] for i in range(3)]

    def hops(offset):
        return sum(min(o, SIDE - o) for o in offset)

    for x, y, z in sorted(itertools.product(range(SIDE), repeat=3), key=hops, reverse=True):
        there = ((steps[2][z] * SIDE + steps[1][y]) * SIDE + steps[0][x]) * 2
        for side in range(2):
            if hops((x, y, z)) == 0 and side == 1:
                continue
            pltpu.make_async_remote_copy(
                src_ref=res_ref,
                dst_ref=fin_ref.at[origin],
                send_sem=fin_send,
                recv_sem=fin_recv,
                device_id=device(partner if hops((x, y, z)) == 0 else there + side),
                device_id_type=MESH,
            ).start()
    others = fin_ref.at[0 : 2 * CHIPS - 1]
    pltpu.make_async_copy(others, others, fin_recv).wait()
    log_prob = fin_ref[0:CHIPS, 0, :] + fin_ref[CHIPS:, 0, :]
    out_ref[0] = log_prob
    out_ref[1] = fin_ref[0:CHIPS, 1, :] + fin_ref[CHIPS:, 1, :]
    mean_ref[0] = jnp.sum(log_prob) * (1.0 / (CHIPS * 2 * rows))

    pltpu.make_async_copy(others, others, fin_send).wait()
    pltpu.make_async_copy(arrived, arrived, stat_send).wait()
    pltpu.make_async_copy(partner_head, partner_head, w_send).wait()
    for event in range(EVENTS):
        wait_event(event, send_sem)


def solution(mesh):
    def local_step(hidden, target, norm_gain, head_weight):
        rows, depth = hidden.shape
        vocab = head_weight.shape[1]
        width = pl.cdiv(vocab, 128) * 128
        half = rows // HALVES
        vmem = pl.BlockSpec(memory_space=pltpu.VMEM)
        dma = pltpu.SemaphoreType.DMA
        out, mean = pl.pallas_call(
            kernel,
            name="head",
            out_shape=(
                jax.ShapeDtypeStruct((2, CHIPS, 2 * rows), jnp.float32),
                jax.ShapeDtypeStruct((1,), jnp.float32),
            ),
            in_specs=[vmem, vmem, vmem, pl.BlockSpec(memory_space=pl.ANY)],
            out_specs=(vmem, pl.BlockSpec(memory_space=pltpu.SMEM)),
            scratch_shapes=[
                pltpu.VMEM((GROUPS, 6, half, depth), jnp.bfloat16),
                pltpu.VMEM((depth, 2 * width), jnp.bfloat16),
                pltpu.VMEM((STAGES, 128, depth), jnp.bfloat16),
                pltpu.VMEM((vocab % 128, depth), jnp.bfloat16),
                pltpu.VMEM((6 * half, 2 * width), jnp.float32),
                pltpu.VMEM((6 * half, 2 * width), jnp.float32),
                pltpu.VMEM((GROUPS, 6, half, 128), jnp.float32),
                pltpu.VMEM((12, half, 128), jnp.float32),
                pltpu.VMEM((CHIPS // 2 + 1, 4, 128), jnp.float32),
                pltpu.VMEM((CHIPS, 4, 128), jnp.float32),
                pltpu.VMEM((2, 128), jnp.float32),
                pltpu.VMEM((2 * CHIPS, 2, 128), jnp.float32),
                dma((EVENTS,)), dma((EVENTS,)), dma((STAGES,)), dma, dma, dma, dma, dma, dma, dma,
            ],
            compiler_params=pltpu.CompilerParams(
                collective_id=0, has_side_effects=True, vmem_limit_bytes=67_000_000
            ),
        )(hidden, norm_gain, target.reshape(CHIPS, 2 * rows), head_weight.T)
        return out[0].reshape(-1), out[1].reshape(-1), mean

    return jax.shard_map(local_step, mesh=mesh, in_specs=(P(("dp", "vp"), None), P("dp"), P(None), P(None, "vp")), out_specs=(P("dp"), P("dp"), P("dp")), check_vma=False)
```

```python
import functools
import itertools

import jax
import jax.numpy as jnp
from jax import lax
from jax.experimental import pallas as pl
from jax.experimental.pallas import tpu as pltpu
from jax.sharding import PartitionSpec as P

NORM_EPS = 1e-6
MESH = pl.DeviceIdType.MESH
SIDE = 4
CHIPS = SIDE**3
OWN = CHIPS - 1
LOW = -3.0e38
DIRS = ((1, 0, 0), (0, 1, 0), (0, 0, 1), (-1, 0, 0), (0, -1, 0), (0, 0, -1))
FULL = 10

PARENT = (
    63, 63, 63, 63, 63, 63, 4, 0, 4, 3, 4, 0, 2, 3, 3, 4, 5, 5, 7, 2, 6, 5, 9, 1, 11, 17, 12, 16, 11, 16, 10, 19,
    9, 8, 16, 7, 26, 12, 14, 19, 15, 13, 35, 18, 30, 29, 28, 35, 28, 36, 31, 31, 26, 41, 46, 41, 43, 39, 32, 46, 52, 49, 51,
)
HALVES = 2
EVENTS = HALVES * (FULL + 1)
GROUPS = EVENTS
AHEAD = 4
STAGES = 4
WIDE = 512


def offsets():
    out = {OWN: (0, 0, 0)}
    for j, parent in enumerate(PARENT):
        out[j] = tuple((a + b) % SIDE for a, b in zip(out[parent], DIRS[j % 6]))
    return out


OFFSET = offsets()
FARTHEST = (SIDE // 2,) * 3


def pieces_of(slot):
    return range(6 * slot, min(6 * slot + 6, OWN))


def place(piece, c):
    if piece == OWN:
        return GROUPS - 1, c
    if piece >= 6 * FULL:
        return HALVES * FULL, piece - 6 * FULL + 3 * c
    return HALVES * (piece // 6) + c, piece % 6


def kernel(hidden_hbm, gain_hbm, target_hbm, head_ref, out_ref, mean_ref, hidden_ref, gain_ref, target_ref, x_ref, w_ref, stage_ref, rest_ref, za_ref, zb_ref,
           tgt_ref, pack_ref, mine_ref, stat_ref, res_ref, fin_ref, send_sem, recv_sem, stage_sem, rest_sem, w_send, w_recv,
           stat_send, stat_recv, fin_send, fin_recv, in_sem):
    rows, depth = hidden_ref.shape
    half = rows // HALVES
    vocab = head_ref.shape[0]
    tiles = pl.cdiv(vocab, 128)
    width = tiles * 128
    me = lax.axis_index("vp")
    group = lax.axis_index("dp")
    core = lax.rem(me, 2)
    chip = me // 2
    coords = (lax.rem(chip, SIDE), lax.rem(chip // SIDE, SIDE), chip // (SIDE * SIDE))
    sign = 1 - 2 * core
    partner = me + sign

    def device(there):
        return (group, there)

    def chip_at(offset):
        c = [lax.rem(coords[i] + sign * offset[i] + 2 * SIDE, SIDE) for i in range(3)]
        return (c[2] * SIDE + c[1]) * SIDE + c[0]

    neighbours = [chip_at(d) * 2 + core for d in DIRS]

    def behind(piece):
        return chip_at([-o for o in OFFSET[piece]])

    def merger(piece):
        return chip_at([SIDE // 2 - o for o in OFFSET[piece]])

    barrier = pltpu.get_barrier_semaphore()
    for there in (*neighbours, partner):
        pl.semaphore_signal(barrier, inc=1, device_id=device(there), device_id_type=MESH)

    def stage_copy(n):
        return pltpu.make_async_copy(head_ref.at[128 * n : 128 * n + 128], stage_ref.at[n % STAGES], stage_sem.at[n % STAGES])

    whole = vocab // 128
    inputs = [
        pltpu.make_async_copy(src, dst, in_sem.at[i])
        for i, (src, dst) in enumerate(((hidden_hbm, hidden_ref), (gain_hbm, gain_ref), (target_hbm, target_ref)))
    ]
    for copy in inputs:
        copy.start()
    for n in range(STAGES):
        stage_copy(n).start()
    rest_copy = pltpu.make_async_copy(head_ref.at[128 * whole : vocab], rest_ref, rest_sem)
    rest_copy.start()

    for copy in inputs:
        copy.wait()
    h = hidden_ref[...].astype(jnp.float32)
    inv_rms = lax.rsqrt(jnp.mean(h * h, axis=-1, keepdims=True) + NORM_EPS)
    normed = (h * inv_rms * gain_ref[...].astype(jnp.float32)).astype(jnp.bfloat16)
    for c in range(HALVES):
        x_ref[GROUPS - 1, c] = normed[c * half : (c + 1) * half]

    pl.semaphore_wait(barrier, 7)

    def send_event(event):
        c = event % HALVES
        for piece in pieces_of(event // HALVES):
            pltpu.make_async_remote_copy(
                src_ref=x_ref.at[place(PARENT[piece], c)],
                dst_ref=x_ref.at[place(piece, c)],
                send_sem=send_sem.at[event],
                recv_sem=recv_sem.at[event],
                device_id=device(neighbours[piece % 6]),
                device_id_type=MESH,
            ).start()

    def wait_event(event, sem):
        ps = pieces_of(event // HALVES)
        g, d = place(ps.start, event % HALVES)
        block = x_ref.at[g, d : d + len(ps)]
        pltpu.make_async_copy(block, block, sem.at[event]).wait()

    for event in range(HALVES):
        send_event(event)

    def head_copy(n):
        return pltpu.make_async_remote_copy(
            src_ref=w_ref.at[:, 128 * n : 128 * n + 128],
            dst_ref=w_ref.at[:, width + 128 * n : width + 128 * n + 128],
            send_sem=w_send,
            recv_sem=w_recv,
            device_id=device(partner),
            device_id_type=MESH,
        )

    for n in range(tiles):
        if n < whole:
            stage_copy(n).wait()
        else:
            rest_copy.wait()
            stage_ref[n % STAGES, 0 : vocab - 128 * whole] = rest_ref[...]

        def turn(k, carry, n=n):
            for u in range(4):
                at = pl.multiple_of((4 * k + u) * 128, 128)
                w_ref[pl.ds(at, 128), 128 * n : 128 * n + 128] = stage_ref[n % STAGES, :, pl.ds(at, 128)].T
            return carry

        lax.fori_loop(0, depth // 512, turn, 0)
        if n + STAGES < whole:
            stage_copy(n + STAGES).start()
        if n:
            head_copy(n - 1).start()

    lane_ids = lax.broadcasted_iota(jnp.int32, (half, 128), 1)
    row_ids = lax.broadcasted_iota(jnp.int32, (half, 128), 0)
    lanes = lane_ids.astype(jnp.float32)
    last_ok = lane_ids < vocab - (tiles - 1) * 128

    def targets(piece):
        row = target_ref[pl.ds(behind(piece), 1), :].astype(jnp.float32)
        for c in range(HALVES):
            hit = lane_ids == row_ids + (core * rows + c * half)
            column = jnp.sum(jnp.where(hit, row, 0.0), axis=1, keepdims=True)
            tgt_ref[place(piece, c)] = column - lanes

    for piece in range(CHIPS):
        targets(piece)
        if piece == 0:
            head_copy(tiles - 1).start()

    def comm(event):
        wait_event(event, recv_sem)
        if event < HALVES:
            send_event(event + HALVES)
        if event + AHEAD < EVENTS:
            send_event(event + AHEAD)

    comm(0)
    comm(1)
    partner_head = w_ref.at[:, width : 2 * width]
    pltpu.make_async_copy(partner_head, partner_head, w_recv).wait()

    base = [(me * vocab).astype(jnp.float32), (partner * vocab).astype(jnp.float32)]

    def strip_stats(z_ref, g, d, pack_at):
        def tile(b, k):
            return z_ref[d * half : (d + 1) * half, (b * tiles + k) * 128 : (b * tiles + k + 1) * 128]

        def masked(k, v, other):
            return jnp.where(last_ok, v, other) if k == tiles - 1 else v

        top = tile(0, 0)
        for b in range(2):
            for k in range(tiles):
                top = jnp.maximum(top, masked(k, tile(b, k), LOW))
        total = jnp.zeros_like(top)
        moment = jnp.zeros_like(top)
        picked = jnp.zeros_like(top)
        for b in range(2):
            where = tgt_ref[g, d] - base[b]
            for k in range(tiles):
                z = tile(b, k)
                shifted = z - top
                e = jnp.exp(shifted)
                total += masked(k, e, 0.0)
                moment += masked(k, e * shifted, 0.0)
                hit = where == float(128 * k)
                if k == tiles - 1:
                    hit = hit & last_ok
                picked = jnp.where(hit, z, picked)
        row_top = jnp.max(top, axis=1, keepdims=True)
        drop = top - row_top
        scale = jnp.exp(drop)
        row_moment = jnp.sum((moment + total * drop) * scale, axis=1, keepdims=True)
        row_total = jnp.sum(total * scale, axis=1, keepdims=True)
        row_picked = jnp.sum(picked, axis=1, keepdims=True)
        packed = jnp.where(lane_ids == 0, row_top, jnp.where(lane_ids == 1, row_total, jnp.where(lane_ids == 2, row_moment, row_picked)))
        pack_ref[pack_at] = packed

    def part(g, z_ref, before, other_ref, pack_at):
        x = x_ref[g].reshape(6 * half, depth)
        for n in range(2 * width // WIDE):
            at = slice(n * WIDE, (n + 1) * WIDE)
            for d in range(2 * n, min(2 * n + 2, 6)):
                strip_stats(other_ref, before, d, pack_at(d))
            z_ref[:, at] = jnp.dot(x, w_ref[:, at], preferred_element_type=jnp.float32)

    def flush(pairs, first_pair):
        for i in range(pairs):
            block = pack_ref[4 * i : 4 * i + 4].reshape(2 * rows, 128)
            mine_ref[first_pair + i] = block.T[0:4, :]

    def stat_copy(piece):
        return pltpu.make_async_remote_copy(
            src_ref=mine_ref.at[CHIPS // 2 if piece == OWN else piece // 2],
            dst_ref=stat_ref.at[piece],
            send_sem=stat_send,
            recv_sem=stat_recv,
            device_id=device(merger(piece) * 2 + core),
            device_id_type=MESH,
        )

    def send_stats(pieces):
        for piece in pieces:
            if OFFSET[piece] == FARTHEST:
                stat_ref[piece] = mine_ref[piece // 2]
            else:
                stat_copy(piece).start()

    def at_turn(turn, first, last, what):
        for t in range(first, last):
            pl.when(turn == t)(functools.partial(what, t))

    def step(turn, carry):
        def before_first(t):
            comm(2 * t - 1)

        def before_second(t):
            comm(2 * t)
            if t == FULL:
                comm(2 * t + 1)
            if t == FULL - 2:
                send_stats([*range(18), OWN])
            if t == FULL - 1:
                send_stats(range(18, 42))
            if t == FULL:
                send_stats(range(42, 54))

        at_turn(turn, 2, FULL + 1, before_first)
        first = jnp.where(turn == 0, GROUPS - 1, 2 * turn - 1)
        part(first, za_ref, jnp.maximum(2 * turn - 2, 0), zb_ref, lambda d: 2 * d)
        at_turn(turn, 1, FULL + 1, before_second)
        part(2 * turn, zb_ref, first, za_ref, lambda d: jnp.where(turn == 0, d, 2 * d + 1))

        @pl.when(turn > 0)
        def _():
            flush(3, 3 * (turn - 1))

        @pl.when(turn == 0)
        def _():
            pack_ref[2] = pack_ref[0]
            pack_ref[3] = pack_ref[1]
            flush(1, CHIPS // 2)

        return carry

    lax.fori_loop(0, FULL + 1, step, 0)
    send_stats(pieces_of(FULL - 1))
    for d in range(6):
        strip_stats(zb_ref, HALVES * FULL, d, 2 * (d % 3) + d // 3)
    flush(2, 3 * FULL)
    send_stats(pieces_of(FULL))

    arrived = stat_ref.at[0 : CHIPS - 1]
    pltpu.make_async_copy(arrived, arrived, stat_recv).wait()
    piece_id = lax.broadcasted_iota(jnp.int32, (CHIPS, 128), 0)
    lane = lax.broadcasted_iota(jnp.int32, (CHIPS, 128), 1)
    ok = lax.rem(piece_id, 2) == lane // rows

    def folded(v, op):
        return op(v, pltpu.roll(v, rows, 1))

    tops = jnp.where(ok, stat_ref[:, 0, :], LOW)
    top = jnp.max(tops, axis=0, keepdims=True)
    top = folded(top, jnp.maximum)
    drop = tops - top
    scale = jnp.exp(drop)
    totals = stat_ref[:, 1, :]
    total = folded(jnp.sum(jnp.where(ok, totals * scale, 0.0), axis=0, keepdims=True), jnp.add)
    moments = (stat_ref[:, 2, :] + totals * drop) * scale
    moment = folded(jnp.sum(jnp.where(ok, moments, 0.0), axis=0, keepdims=True), jnp.add)
    picked = folded(jnp.sum(jnp.where(ok, stat_ref[:, 3, :], 0.0), axis=0, keepdims=True), jnp.add)
    log_total = jnp.log(total)
    low = lax.broadcasted_iota(jnp.int32, (1, 128), 1) < rows
    res_ref[...] = jnp.where(low, picked - top - log_total, log_total - moment / total)

    origin = core * CHIPS + merger(OWN)
    fin_ref[origin] = res_ref[...]
    steps = [[lax.rem(coords[i] + k, SIDE) for k in range(SIDE)] for i in range(3)]

    def hops(offset):
        return sum(min(o, SIDE - o) for o in offset)

    for x, y, z in sorted(itertools.product(range(SIDE), repeat=3), key=hops, reverse=True):
        there = ((steps[2][z] * SIDE + steps[1][y]) * SIDE + steps[0][x]) * 2
        for side in range(2):
            if hops((x, y, z)) == 0 and side == 1:
                continue
            pltpu.make_async_remote_copy(
                src_ref=res_ref,
                dst_ref=fin_ref.at[origin],
                send_sem=fin_send,
                recv_sem=fin_recv,
                device_id=device(partner if hops((x, y, z)) == 0 else there + side),
                device_id_type=MESH,
            ).start()
    others = fin_ref.at[0 : 2 * CHIPS - 1]
    pltpu.make_async_copy(others, others, fin_recv).wait()
    first, second = fin_ref[0:CHIPS, 0, :], fin_ref[CHIPS:, 0, :]
    low = lane < rows
    log_prob = jnp.where(low, first, pltpu.roll(second, rows, 1))
    out_ref[0] = log_prob
    out_ref[1] = jnp.where(low, pltpu.roll(first, rows, 1), second)
    mean_ref[0] = jnp.sum(log_prob) * (1.0 / (CHIPS * 2 * rows))

    pltpu.make_async_copy(others, others, fin_send).wait()
    pltpu.make_async_copy(arrived, arrived, stat_send).wait()
    pltpu.make_async_copy(partner_head, partner_head, w_send).wait()
    for event in range(EVENTS):
        wait_event(event, send_sem)


def solution(mesh):
    def local_step(hidden, target, norm_gain, head_weight):
        rows, depth = hidden.shape
        vocab = head_weight.shape[1]
        width = pl.cdiv(vocab, 128) * 128
        half = rows // HALVES
        vmem = pl.BlockSpec(memory_space=pltpu.VMEM)
        dma = pltpu.SemaphoreType.DMA
        out, mean = pl.pallas_call(
            kernel,
            name="head",
            out_shape=(
                jax.ShapeDtypeStruct((2, CHIPS, 2 * rows), jnp.float32),
                jax.ShapeDtypeStruct((1,), jnp.float32),
            ),
            in_specs=[pl.BlockSpec(memory_space=pl.ANY)] * 4,
            out_specs=(vmem, pl.BlockSpec(memory_space=pltpu.SMEM)),
            scratch_shapes=[
                pltpu.VMEM((rows, depth), jnp.bfloat16),
                pltpu.VMEM((depth,), jnp.bfloat16),
                pltpu.VMEM((CHIPS, 2 * rows), jnp.int32),
                pltpu.VMEM((GROUPS, 6, half, depth), jnp.bfloat16),
                pltpu.VMEM((depth, 2 * width), jnp.bfloat16),
                pltpu.VMEM((STAGES, 128, depth), jnp.bfloat16),
                pltpu.VMEM((vocab % 128, depth), jnp.bfloat16),
                pltpu.VMEM((6 * half, 2 * width), jnp.float32),
                pltpu.VMEM((6 * half, 2 * width), jnp.float32),
                pltpu.VMEM((GROUPS, 6, half, 128), jnp.float32),
                pltpu.VMEM((12, half, 128), jnp.float32),
                pltpu.VMEM((CHIPS // 2 + 1, 4, 128), jnp.float32),
                pltpu.VMEM((CHIPS, 4, 128), jnp.float32),
                pltpu.VMEM((1, 128), jnp.float32),
                pltpu.VMEM((2 * CHIPS, 1, 128), jnp.float32),
                dma((EVENTS,)), dma((EVENTS,)), dma((STAGES,)), dma, dma, dma, dma, dma, dma, dma,
                dma((3,)),
            ],
            compiler_params=pltpu.CompilerParams(
                collective_id=0,
                has_side_effects=True,
                vmem_limit_bytes=67_000_000,
            ),
        )(hidden, norm_gain, target.reshape(CHIPS, 2 * rows), head_weight.T)
        return out[0].reshape(-1), out[1].reshape(-1), mean

    return jax.shard_map(local_step, mesh=mesh, in_specs=(P(("dp", "vp"), None), P("dp"), P(None), P(None, "vp")), out_specs=(P("dp"), P("dp"), P("dp")), check_vma=False)
```

```python
import functools
import itertools

import jax
import jax.numpy as jnp
from jax import lax
from jax.experimental import pallas as pl
from jax.experimental.pallas import tpu as pltpu
from jax.sharding import PartitionSpec as P

NORM_EPS = 1e-6
MESH = pl.DeviceIdType.MESH
SIDE = 4
CHIPS = SIDE**3
OWN = CHIPS - 1
LOW = -3.0e38
DIRS = ((1, 0, 0), (0, 1, 0), (0, 0, 1), (-1, 0, 0), (0, -1, 0), (0, 0, -1))
FULL = 10

PARENT = (
    63, 63, 63, 63, 63, 63, 4, 0, 4, 3, 4, 0, 2, 3, 3, 4, 5, 5, 7, 2, 6, 5, 9, 1, 11, 17, 12, 16, 11, 16, 10, 19,
    9, 8, 16, 7, 26, 12, 14, 19, 15, 13, 35, 18, 30, 29, 28, 35, 28, 36, 31, 31, 26, 41, 46, 41, 43, 39, 32, 46, 52, 49, 51,
)
HALVES = 2
EVENTS = HALVES * (FULL + 1)
GROUPS = EVENTS
AHEAD = 4
STAGES = 4
WIDE = 512


def offsets():
    out = {OWN: (0, 0, 0)}
    for j, parent in enumerate(PARENT):
        out[j] = tuple((a + b) % SIDE for a, b in zip(out[parent], DIRS[j % 6]))
    return out


OFFSET = offsets()
FARTHEST = (SIDE // 2,) * 3


def pieces_of(slot):
    return range(6 * slot, min(6 * slot + 6, OWN))


def place(piece, c):
    if piece == OWN:
        return GROUPS - 1, c
    if piece >= 6 * FULL:
        return HALVES * FULL, piece - 6 * FULL + 3 * c
    return HALVES * (piece // 6) + c, piece % 6


def kernel(hidden_hbm, gain_hbm, target_hbm, head_ref, out_ref, mean_ref, hidden_ref, gain_ref, target_ref, x_ref, w_ref, stage_ref, rest_ref, za_ref, zb_ref,
           tgt_ref, pack_ref, mine_ref, stat_ref, res_ref, fin_ref, send_sem, recv_sem, stage_sem, rest_sem, w_send, w_recv,
           stat_send, stat_recv, fin_send, fin_recv, in_sem):
    rows, depth = hidden_ref.shape
    half = rows // HALVES
    vocab = head_ref.shape[0]
    tiles = pl.cdiv(vocab, 128)
    width = tiles * 128
    me = lax.axis_index("vp")
    group = lax.axis_index("dp")
    core = lax.rem(me, 2)
    chip = me // 2
    coords = (lax.rem(chip, SIDE), lax.rem(chip // SIDE, SIDE), chip // (SIDE * SIDE))
    sign = 1 - 2 * core
    partner = me + sign

    def device(there):
        return (group, there)

    def chip_at(offset):
        c = [lax.rem(coords[i] + sign * offset[i] + 2 * SIDE, SIDE) for i in range(3)]
        return (c[2] * SIDE + c[1]) * SIDE + c[0]

    neighbours = [chip_at(d) * 2 + core for d in DIRS]

    def behind(piece):
        return chip_at([-o for o in OFFSET[piece]])

    def merger(piece):
        return chip_at([SIDE // 2 - o for o in OFFSET[piece]])

    barrier = pltpu.get_barrier_semaphore()
    for there in (*neighbours, partner):
        pl.semaphore_signal(barrier, inc=1, device_id=device(there), device_id_type=MESH)

    def stage_copy(n):
        return pltpu.make_async_copy(head_ref.at[128 * n : 128 * n + 128], stage_ref.at[n % STAGES], stage_sem.at[n % STAGES])

    whole = vocab // 128
    inputs = [
        pltpu.make_async_copy(src, dst, in_sem.at[i])
        for i, (src, dst) in enumerate(((hidden_hbm, hidden_ref), (gain_hbm, gain_ref), (target_hbm, target_ref)))
    ]
    for copy in inputs:
        copy.start()
    for n in range(STAGES):
        stage_copy(n).start()
    rest_copy = pltpu.make_async_copy(head_ref.at[128 * whole : vocab], rest_ref, rest_sem)
    rest_copy.start()

    for copy in inputs:
        copy.wait()
    h = hidden_ref[...].astype(jnp.float32)
    inv_rms = lax.rsqrt(jnp.mean(h * h, axis=-1, keepdims=True) + NORM_EPS)
    normed = (h * inv_rms * gain_ref[...].astype(jnp.float32)).astype(jnp.bfloat16)
    for c in range(HALVES):
        x_ref[GROUPS - 1, c] = normed[c * half : (c + 1) * half]

    pl.semaphore_wait(barrier, 7)

    def send_event(event):
        c = event % HALVES
        for piece in pieces_of(event // HALVES):
            pltpu.make_async_remote_copy(
                src_ref=x_ref.at[place(PARENT[piece], c)],
                dst_ref=x_ref.at[place(piece, c)],
                send_sem=send_sem.at[event],
                recv_sem=recv_sem.at[event],
                device_id=device(neighbours[piece % 6]),
                device_id_type=MESH,
            ).start()

    def wait_event(event, sem):
        ps = pieces_of(event // HALVES)
        g, d = place(ps.start, event % HALVES)
        block = x_ref.at[g, d : d + len(ps)]
        pltpu.make_async_copy(block, block, sem.at[event]).wait()

    for event in range(HALVES):
        send_event(event)

    def head_copy(n):
        return pltpu.make_async_remote_copy(
            src_ref=w_ref.at[:, 128 * n : 128 * n + 128],
            dst_ref=w_ref.at[:, width + 128 * n : width + 128 * n + 128],
            send_sem=w_send,
            recv_sem=w_recv,
            device_id=device(partner),
            device_id_type=MESH,
        )

    for n in range(tiles):
        if n < whole:
            stage_copy(n).wait()
        else:
            rest_copy.wait()
            stage_ref[n % STAGES, 0 : vocab - 128 * whole] = rest_ref[...]

        def turn(k, carry, n=n):
            for u in range(4):
                at = pl.multiple_of((4 * k + u) * 128, 128)
                w_ref[pl.ds(at, 128), 128 * n : 128 * n + 128] = stage_ref[n % STAGES, :, pl.ds(at, 128)].T
            return carry

        lax.fori_loop(0, depth // 512, turn, 0)
        if n + STAGES < whole:
            stage_copy(n + STAGES).start()
        if n:
            head_copy(n - 1).start()

    lane_ids = lax.broadcasted_iota(jnp.int32, (half, 128), 1)
    row_ids = lax.broadcasted_iota(jnp.int32, (half, 128), 0)
    lanes = lane_ids.astype(jnp.float32)
    last_ok = lane_ids < vocab - (tiles - 1) * 128

    def targets(piece):
        row = target_ref[pl.ds(behind(piece), 1), :].astype(jnp.float32)
        for c in range(HALVES):
            hit = lane_ids == row_ids + (core * rows + c * half)
            column = jnp.sum(jnp.where(hit, row, 0.0), axis=1, keepdims=True)
            tgt_ref[place(piece, c)] = column - lanes

    for piece in range(CHIPS):
        targets(piece)
        if piece == 0:
            head_copy(tiles - 1).start()

    def comm(event):
        wait_event(event, recv_sem)
        if event < HALVES:
            send_event(event + HALVES)
        if event + AHEAD < EVENTS:
            send_event(event + AHEAD)

    comm(0)
    comm(1)
    partner_head = w_ref.at[:, width : 2 * width]
    pltpu.make_async_copy(partner_head, partner_head, w_recv).wait()

    base = [(me * vocab).astype(jnp.float32), (partner * vocab).astype(jnp.float32)]

    def strip_stats(z_ref, g, d, pack_at):
        def tile(b, k):
            return z_ref[d * half : (d + 1) * half, (b * tiles + k) * 128 : (b * tiles + k + 1) * 128]

        def masked(k, v, other):
            return jnp.where(last_ok, v, other) if k == tiles - 1 else v

        top = tile(0, 0)
        for b in range(2):
            for k in range(tiles):
                top = jnp.maximum(top, masked(k, tile(b, k), LOW))
        total = jnp.zeros_like(top)
        moment = jnp.zeros_like(top)
        picked = jnp.zeros_like(top)
        for b in range(2):
            where = tgt_ref[g, d] - base[b]
            for k in range(tiles):
                z = tile(b, k)
                shifted = z - top
                e = jnp.exp(shifted)
                total += masked(k, e, 0.0)
                moment += masked(k, e * shifted, 0.0)
                hit = where == float(128 * k)
                if k == tiles - 1:
                    hit = hit & last_ok
                picked = jnp.where(hit, z, picked)
        row_top = jnp.max(top, axis=1, keepdims=True)
        drop = top - row_top
        scale = jnp.exp(drop)
        row_moment = jnp.sum((moment + total * drop) * scale, axis=1, keepdims=True)
        row_total = jnp.sum(total * scale, axis=1, keepdims=True)
        row_picked = jnp.sum(picked, axis=1, keepdims=True)
        packed = jnp.where(lane_ids == 0, row_top, jnp.where(lane_ids == 1, row_total, jnp.where(lane_ids == 2, row_moment, row_picked)))
        pack_ref[pack_at] = packed

    def part(g, z_ref, before, other_ref, pack_at):
        x = x_ref[g].reshape(6 * half, depth)
        for n in range(2 * width // WIDE):
            at = slice(n * WIDE, (n + 1) * WIDE)
            for d in range(2 * n, min(2 * n + 2, 6)):
                strip_stats(other_ref, before, d, pack_at(d))
            z_ref[:, at] = jnp.dot(x, w_ref[:, at], preferred_element_type=jnp.float32)

    low = lax.broadcasted_iota(jnp.int32, (1, 128), 1) < rows

    def flush(pieces):
        for i in range(0, len(pieces), 2):
            block = pack_ref[2 * i : 2 * i + 4].reshape(2 * rows, 128).T
            turned = pltpu.roll(block[0:8, :], rows, 1)
            for j, piece in enumerate(pieces[i : i + 2]):
                left, right = (block, turned) if j == 0 else (turned, block)
                mine_ref[piece, 0:1] = jnp.where(low, left[0:1, :], right[1:2, :])
                mine_ref[piece, 1:2] = jnp.where(low, left[2:3, :], right[3:4, :])

    def stat_copy(piece):
        return pltpu.make_async_remote_copy(
            src_ref=mine_ref.at[piece],
            dst_ref=stat_ref.at[piece],
            send_sem=stat_send,
            recv_sem=stat_recv,
            device_id=device(merger(piece) * 2 + core),
            device_id_type=MESH,
        )

    def send_stats(pieces):
        for piece in pieces:
            if OFFSET[piece] == FARTHEST:
                stat_ref[piece] = mine_ref[piece]
            else:
                stat_copy(piece).start()

    def at_turn(turn, first, last, what):
        for t in range(first, last):
            pl.when(turn == t)(functools.partial(what, t))

    def step(turn, carry):
        def before_first(t):
            comm(2 * t - 1)

        def before_second(t):
            comm(2 * t)
            if t == FULL:
                comm(2 * t + 1)
            if t == FULL - 2:
                send_stats([*range(18), OWN])
            if t == FULL - 1:
                send_stats(range(18, 42))
            if t == FULL:
                send_stats(range(42, 54))

        at_turn(turn, 2, FULL + 1, before_first)
        first = jnp.where(turn == 0, GROUPS - 1, 2 * turn - 1)
        part(first, za_ref, jnp.maximum(2 * turn - 2, 0), zb_ref, lambda d: 2 * d)
        at_turn(turn, 1, FULL + 1, before_second)
        part(2 * turn, zb_ref, first, za_ref, lambda d: jnp.where(turn == 0, d, 2 * d + 1))

        @pl.when(turn > 0)
        def _():
            flush([6 * (turn - 1) + i for i in range(6)])

        @pl.when(turn == 0)
        def _():
            flush([OWN])

        return carry

    lax.fori_loop(0, FULL + 1, step, 0)
    send_stats(pieces_of(FULL - 1))
    for d in range(6):
        strip_stats(zb_ref, HALVES * FULL, d, 2 * (d % 3) + d // 3)
    flush(pieces_of(FULL))
    send_stats(pieces_of(FULL))

    arrived = stat_ref.at[0 : CHIPS - 1]
    pltpu.make_async_copy(arrived, arrived, stat_recv).wait()
    tops, moments = stat_ref[:, 0, :], stat_ref[:, 1, :]
    totals, picks = pltpu.roll(tops, rows, 1), pltpu.roll(moments, rows, 1)
    top = jnp.max(tops, axis=0, keepdims=True)
    drop = tops - top
    scale = jnp.exp(drop)
    total = jnp.sum(totals * scale, axis=0, keepdims=True)
    moment = jnp.sum((moments + totals * drop) * scale, axis=0, keepdims=True)
    picked = jnp.sum(picks, axis=0, keepdims=True)
    log_total = jnp.log(total)
    res_ref[...] = jnp.where(low, picked - top - log_total, pltpu.roll(log_total - moment / total, rows, 1))

    origin = core * CHIPS + merger(OWN)
    fin_ref[origin] = res_ref[...]
    steps = [[lax.rem(coords[i] + k, SIDE) for k in range(SIDE)] for i in range(3)]

    def hops(offset):
        return sum(min(o, SIDE - o) for o in offset)

    for x, y, z in sorted(itertools.product(range(SIDE), repeat=3), key=hops, reverse=True):
        there = ((steps[2][z] * SIDE + steps[1][y]) * SIDE + steps[0][x]) * 2
        for side in range(2):
            if hops((x, y, z)) == 0 and side == 1:
                continue
            pltpu.make_async_remote_copy(
                src_ref=res_ref,
                dst_ref=fin_ref.at[origin],
                send_sem=fin_send,
                recv_sem=fin_recv,
                device_id=device(partner if hops((x, y, z)) == 0 else there + side),
                device_id_type=MESH,
            ).start()
    others = fin_ref.at[0 : 2 * CHIPS - 1]
    pltpu.make_async_copy(partner_head, partner_head, w_send).wait()
    for event in range(EVENTS):
        wait_event(event, send_sem)
    pltpu.make_async_copy(arrived, arrived, stat_send).wait()
    pltpu.make_async_copy(others, others, fin_send).wait()

    pltpu.make_async_copy(others, others, fin_recv).wait()
    first, second = fin_ref[0:CHIPS, 0, :], fin_ref[CHIPS:, 0, :]
    log_prob = jnp.where(low, first, pltpu.roll(second, rows, 1))
    out_ref[0] = log_prob
    out_ref[1] = jnp.where(low, pltpu.roll(first, rows, 1), second)
    mean_ref[0] = jnp.sum(log_prob) * (1.0 / (CHIPS * 2 * rows))


def solution(mesh):
    def local_step(hidden, target, norm_gain, head_weight):
        rows, depth = hidden.shape
        vocab = head_weight.shape[1]
        width = pl.cdiv(vocab, 128) * 128
        half = rows // HALVES
        vmem = pl.BlockSpec(memory_space=pltpu.VMEM)
        dma = pltpu.SemaphoreType.DMA
        out, mean = pl.pallas_call(
            kernel,
            name="head",
            out_shape=(
                pltpu.VMEM((2, CHIPS, 2 * rows), jnp.float32),
                jax.ShapeDtypeStruct((1,), jnp.float32),
            ),
            in_specs=[pl.BlockSpec(memory_space=pl.ANY)] * 4,
            out_specs=(vmem, pl.BlockSpec(memory_space=pltpu.SMEM)),
            scratch_shapes=[
                pltpu.VMEM((rows, depth), jnp.bfloat16),
                pltpu.VMEM((depth,), jnp.bfloat16),
                pltpu.VMEM((CHIPS, 2 * rows), jnp.int32),
                pltpu.VMEM((GROUPS, 6, half, depth), jnp.bfloat16),
                pltpu.VMEM((depth, 2 * width), jnp.bfloat16),
                pltpu.VMEM((STAGES, 128, depth), jnp.bfloat16),
                pltpu.VMEM((vocab % 128, depth), jnp.bfloat16),
                pltpu.VMEM((6 * half, 2 * width), jnp.float32),
                pltpu.VMEM((6 * half, 2 * width), jnp.float32),
                pltpu.VMEM((GROUPS, 6, half, 128), jnp.float32),
                pltpu.VMEM((12, half, 128), jnp.float32),
                pltpu.VMEM((CHIPS, 2, 128), jnp.float32),
                pltpu.VMEM((CHIPS, 2, 128), jnp.float32),
                pltpu.VMEM((1, 128), jnp.float32),
                pltpu.VMEM((2 * CHIPS, 1, 128), jnp.float32),
                dma((EVENTS,)), dma((EVENTS,)), dma((STAGES,)), dma, dma, dma, dma, dma, dma, dma,
                dma((3,)),
            ],
            compiler_params=pltpu.CompilerParams(
                collective_id=0,
                has_side_effects=True,
                vmem_limit_bytes=66_000_000,
            ),
        )(hidden, norm_gain, target.reshape(CHIPS, 2 * rows), head_weight.T)
        return out[0].reshape(-1), out[1].reshape(-1), mean

    return jax.shard_map(local_step, mesh=mesh, in_specs=(P(("dp", "vp"), None), P("dp"), P(None), P(None, "vp")), out_specs=(P("dp"), P("dp"), P("dp")), check_vma=False)
```

```python
import functools
import itertools

import jax
import jax.numpy as jnp
from jax import lax
from jax.experimental import pallas as pl
from jax.experimental.pallas import tpu as pltpu
from jax.sharding import PartitionSpec as P

NORM_EPS = 1e-6
MESH = pl.DeviceIdType.MESH
SIDE = 4
CHIPS = SIDE**3
OWN = CHIPS - 1
LOW = -3.0e38
DIRS = ((1, 0, 0), (0, 1, 0), (0, 0, 1), (-1, 0, 0), (0, -1, 0), (0, 0, -1))
FULL = 10

PARENT = (
    63, 63, 63, 63, 63, 63, 4, 0, 4, 3, 4, 0, 2, 3, 3, 4, 5, 5, 7, 2, 6, 5, 9, 1, 11, 17, 12, 16, 11, 16, 10, 19,
    9, 8, 16, 7, 26, 12, 14, 19, 15, 13, 35, 18, 30, 29, 28, 35, 28, 36, 31, 31, 26, 41, 46, 41, 43, 39, 32, 46, 52, 49, 51,
)
HALVES = 2
EVENTS = HALVES * (FULL + 1)
GROUPS = EVENTS
AHEAD = 4
STAGES = 4
WIDE = 512


def offsets():
    out = {OWN: (0, 0, 0)}
    for j, parent in enumerate(PARENT):
        out[j] = tuple((a + b) % SIDE for a, b in zip(out[parent], DIRS[j % 6]))
    return out


OFFSET = offsets()
FARTHEST = (SIDE // 2,) * 3


def pieces_of(slot):
    return range(6 * slot, min(6 * slot + 6, OWN))


def place(piece, c):
    if piece == OWN:
        return GROUPS - 1, c
    if piece >= 6 * FULL:
        return HALVES * FULL, piece - 6 * FULL + 3 * c
    return HALVES * (piece // 6) + c, piece % 6


def kernel(hidden_hbm, gain_hbm, target_hbm, head_ref, out_ref, hidden_ref, gain_ref, target_ref, x_ref, w_ref, stage_ref, rest_ref, za_ref, zb_ref,
           tgt_ref, pack_ref, mine_ref, stat_ref, res_ref, fin_ref, send_sem, recv_sem, stage_sem, rest_sem, w_send, w_recv,
           stat_send, stat_recv, fin_send, fin_recv, in_sem):
    rows, depth = hidden_ref.shape
    half = rows // HALVES
    vocab = head_ref.shape[0]
    tiles = pl.cdiv(vocab, 128)
    width = tiles * 128
    me = lax.axis_index("vp")
    group = lax.axis_index("dp")
    core = lax.rem(me, 2)
    chip = me // 2
    coords = (lax.rem(chip, SIDE), lax.rem(chip // SIDE, SIDE), chip // (SIDE * SIDE))
    sign = 1 - 2 * core
    partner = me + sign

    def device(there):
        return (group, there)

    def chip_at(offset):
        c = [lax.rem(coords[i] + sign * offset[i] + 2 * SIDE, SIDE) for i in range(3)]
        return (c[2] * SIDE + c[1]) * SIDE + c[0]

    neighbours = [chip_at(d) * 2 + core for d in DIRS]

    def behind(piece):
        return chip_at([-o for o in OFFSET[piece]])

    def merger(piece):
        return chip_at([SIDE // 2 - o for o in OFFSET[piece]])

    barrier = pltpu.get_barrier_semaphore()
    for there in (*neighbours, partner):
        pl.semaphore_signal(barrier, inc=1, device_id=device(there), device_id_type=MESH)

    def stage_copy(n):
        return pltpu.make_async_copy(head_ref.at[128 * n : 128 * n + 128], stage_ref.at[n % STAGES], stage_sem.at[n % STAGES])

    whole = vocab // 128
    gain_copy = pltpu.make_async_copy(gain_hbm, gain_ref, in_sem.at[HALVES])
    target_copy = pltpu.make_async_copy(target_hbm, target_ref, in_sem.at[HALVES + 1])
    hidden_copies = [
        pltpu.make_async_copy(hidden_hbm.at[c * half : (c + 1) * half], hidden_ref.at[c * half : (c + 1) * half], in_sem.at[c])
        for c in range(HALVES)
    ]
    for copy in (gain_copy, *hidden_copies):
        copy.start()

    def send_event(event):
        c = event % HALVES
        for piece in pieces_of(event // HALVES):
            pltpu.make_async_remote_copy(
                src_ref=x_ref.at[place(PARENT[piece], c)],
                dst_ref=x_ref.at[place(piece, c)],
                send_sem=send_sem.at[event],
                recv_sem=recv_sem.at[event],
                device_id=device(neighbours[piece % 6]),
                device_id_type=MESH,
            ).start()

    def wait_event(event, sem):
        ps = pieces_of(event // HALVES)
        g, d = place(ps.start, event % HALVES)
        block = x_ref.at[g, d : d + len(ps)]
        pltpu.make_async_copy(block, block, sem.at[event]).wait()

    gain_copy.wait()
    gain = gain_ref[...].astype(jnp.float32)
    for c in range(HALVES):
        hidden_copies[c].wait()
        if c == HALVES - 1:
            target_copy.start()
            for n in range(STAGES):
                stage_copy(n).start()
            rest_copy = pltpu.make_async_copy(head_ref.at[128 * whole : vocab], rest_ref, rest_sem)
            rest_copy.start()
        h = hidden_ref[c * half : (c + 1) * half].astype(jnp.float32)
        inv_rms = lax.rsqrt(jnp.mean(h * h, axis=-1, keepdims=True) + NORM_EPS)
        x_ref[GROUPS - 1, c] = (h * inv_rms * gain).astype(jnp.bfloat16)
        if c == 0:
            pl.semaphore_wait(barrier, 7)
        send_event(c)

    def head_copy(n):
        return pltpu.make_async_remote_copy(
            src_ref=w_ref.at[:, 128 * n : 128 * n + 128],
            dst_ref=w_ref.at[:, width + 128 * n : width + 128 * n + 128],
            send_sem=w_send,
            recv_sem=w_recv,
            device_id=device(partner),
            device_id_type=MESH,
        )

    for n in range(tiles):
        if n < whole:
            stage_copy(n).wait()
        else:
            rest_copy.wait()
            stage_ref[n % STAGES, 0 : vocab - 128 * whole] = rest_ref[...]

        def turn(k, carry, n=n):
            for u in range(4):
                at = pl.multiple_of((4 * k + u) * 128, 128)
                w_ref[pl.ds(at, 128), 128 * n : 128 * n + 128] = stage_ref[n % STAGES, :, pl.ds(at, 128)].T
            return carry

        lax.fori_loop(0, depth // 512, turn, 0)
        if n + STAGES < whole:
            stage_copy(n + STAGES).start()
        if n:
            head_copy(n - 1).start()

    lane_ids = lax.broadcasted_iota(jnp.int32, (half, 128), 1)
    row_ids = lax.broadcasted_iota(jnp.int32, (half, 128), 0)
    lanes = lane_ids.astype(jnp.float32)
    last_ok = lane_ids < vocab - (tiles - 1) * 128

    def targets(piece):
        row = target_ref[pl.ds(behind(piece), 1), :].astype(jnp.float32)
        for c in range(HALVES):
            hit = lane_ids == row_ids + (core * rows + c * half)
            column = jnp.sum(jnp.where(hit, row, 0.0), axis=1, keepdims=True)
            tgt_ref[place(piece, c)] = column - lanes

    target_copy.wait()
    for piece in range(CHIPS):
        targets(piece)
        if piece == 0:
            head_copy(tiles - 1).start()

    def comm(event):
        wait_event(event, recv_sem)
        if event < HALVES:
            send_event(event + HALVES)
        if event + AHEAD < EVENTS:
            send_event(event + AHEAD)

    comm(0)
    comm(1)
    partner_head = w_ref.at[:, width : 2 * width]
    pltpu.make_async_copy(partner_head, partner_head, w_recv).wait()

    base = [(me * vocab).astype(jnp.float32), (partner * vocab).astype(jnp.float32)]

    def strip_stats(z_ref, g, d, pack_at):
        def tile(b, k):
            return z_ref[d * half : (d + 1) * half, (b * tiles + k) * 128 : (b * tiles + k + 1) * 128]

        def masked(k, v, other):
            return jnp.where(last_ok, v, other) if k == tiles - 1 else v

        top = tile(0, 0)
        for b in range(2):
            for k in range(tiles):
                top = jnp.maximum(top, masked(k, tile(b, k), LOW))
        total = jnp.zeros_like(top)
        moment = jnp.zeros_like(top)
        picked = jnp.zeros_like(top)
        for b in range(2):
            where = tgt_ref[g, d] - base[b]
            for k in range(tiles):
                z = tile(b, k)
                shifted = z - top
                e = jnp.exp(shifted)
                total += masked(k, e, 0.0)
                moment += masked(k, e * shifted, 0.0)
                hit = where == float(128 * k)
                if k == tiles - 1:
                    hit = hit & last_ok
                picked = jnp.where(hit, z, picked)
        row_top = jnp.max(top, axis=1, keepdims=True)
        drop = top - row_top
        scale = jnp.exp(drop)
        row_moment = jnp.sum((moment + total * drop) * scale, axis=1, keepdims=True)
        row_total = jnp.sum(total * scale, axis=1, keepdims=True)
        row_picked = jnp.sum(picked, axis=1, keepdims=True)
        packed = jnp.where(lane_ids == 0, row_top, jnp.where(lane_ids == 1, row_total, jnp.where(lane_ids == 2, row_moment, row_picked)))
        pack_ref[pack_at] = packed

    def part(g, z_ref, before, other_ref, pack_at):
        x = x_ref[g].reshape(6 * half, depth)
        for n in range(2 * width // WIDE):
            at = slice(n * WIDE, (n + 1) * WIDE)
            for d in range(2 * n, min(2 * n + 2, 6)):
                strip_stats(other_ref, before, d, pack_at(d))
            z_ref[:, at] = jnp.dot(x, w_ref[:, at], preferred_element_type=jnp.float32)

    low = lax.broadcasted_iota(jnp.int32, (1, 128), 1) < rows

    def flush(pieces):
        for i in range(0, len(pieces), 2):
            block = pack_ref[2 * i : 2 * i + 4].reshape(2 * rows, 128).T
            turned = pltpu.roll(block[0:8, :], rows, 1)
            for j, piece in enumerate(pieces[i : i + 2]):
                left, right = (block, turned) if j == 0 else (turned, block)
                mine_ref[piece, 0:1] = jnp.where(low, left[0:1, :], right[1:2, :])
                mine_ref[piece, 1:2] = jnp.where(low, left[2:3, :], right[3:4, :])

    def stat_copy(piece):
        return pltpu.make_async_remote_copy(
            src_ref=mine_ref.at[piece],
            dst_ref=stat_ref.at[piece],
            send_sem=stat_send,
            recv_sem=stat_recv,
            device_id=device(merger(piece) * 2 + core),
            device_id_type=MESH,
        )

    def send_stats(pieces):
        for piece in pieces:
            if OFFSET[piece] == FARTHEST:
                stat_ref[piece] = mine_ref[piece]
            else:
                stat_copy(piece).start()

    def at_turn(turn, first, last, what):
        for t in range(first, last):
            pl.when(turn == t)(functools.partial(what, t))

    def step(turn, carry):
        def before_first(t):
            comm(2 * t - 1)

        def before_second(t):
            comm(2 * t)
            if t == FULL:
                comm(2 * t + 1)
            if t == FULL - 2:
                send_stats([*range(18), OWN])
            if t == FULL - 1:
                send_stats(range(18, 42))
            if t == FULL:
                send_stats(range(42, 54))

        at_turn(turn, 2, FULL + 1, before_first)
        first = jnp.where(turn == 0, GROUPS - 1, 2 * turn - 1)
        part(first, za_ref, jnp.maximum(2 * turn - 2, 0), zb_ref, lambda d: 2 * d)
        at_turn(turn, 1, FULL + 1, before_second)
        part(2 * turn, zb_ref, first, za_ref, lambda d: jnp.where(turn == 0, d, 2 * d + 1))

        @pl.when(turn > 0)
        def _():
            flush([6 * (turn - 1) + i for i in range(6)])

        @pl.when(turn == 0)
        def _():
            flush([OWN])

        return carry

    lax.fori_loop(0, FULL + 1, step, 0)
    send_stats(pieces_of(FULL - 1))
    for d in range(6):
        strip_stats(zb_ref, HALVES * FULL, d, 2 * (d % 3) + d // 3)
    flush(pieces_of(FULL))
    send_stats(pieces_of(FULL))

    arrived = stat_ref.at[0 : CHIPS - 1]
    pltpu.make_async_copy(arrived, arrived, stat_recv).wait()
    tops, moments = stat_ref[:, 0, :], stat_ref[:, 1, :]
    totals, picks = pltpu.roll(tops, rows, 1), pltpu.roll(moments, rows, 1)
    top = jnp.max(tops, axis=0, keepdims=True)
    drop = tops - top
    scale = jnp.exp(drop)
    total = jnp.sum(totals * scale, axis=0, keepdims=True)
    moment = jnp.sum((moments + totals * drop) * scale, axis=0, keepdims=True)
    picked = jnp.sum(picks, axis=0, keepdims=True)
    log_total = jnp.log(total)
    res_ref[...] = jnp.where(low, picked - top - log_total, pltpu.roll(log_total - moment / total, rows, 1))

    origin = core * CHIPS + merger(OWN)
    fin_ref[origin] = res_ref[...]
    steps = [[lax.rem(coords[i] + k, SIDE) for k in range(SIDE)] for i in range(3)]

    def hops(offset):
        return sum(min(o, SIDE - o) for o in offset)

    for x, y, z in sorted(itertools.product(range(SIDE), repeat=3), key=hops, reverse=True):
        there = ((steps[2][z] * SIDE + steps[1][y]) * SIDE + steps[0][x]) * 2
        for side in range(2):
            if hops((x, y, z)) == 0 and side == 1:
                continue
            pltpu.make_async_remote_copy(
                src_ref=res_ref,
                dst_ref=fin_ref.at[origin],
                send_sem=fin_send,
                recv_sem=fin_recv,
                device_id=device(partner if hops((x, y, z)) == 0 else there + side),
                device_id_type=MESH,
            ).start()
    others = fin_ref.at[0 : 2 * CHIPS - 1]
    pltpu.make_async_copy(partner_head, partner_head, w_send).wait()
    for event in range(EVENTS):
        wait_event(event, send_sem)
    pltpu.make_async_copy(arrived, arrived, stat_send).wait()
    pltpu.make_async_copy(others, others, fin_send).wait()

    pltpu.make_async_copy(others, others, fin_recv).wait()
    first, second = fin_ref[0:CHIPS, 0, :], fin_ref[CHIPS:, 0, :]
    log_prob = jnp.where(low, first, pltpu.roll(second, rows, 1))
    out_ref[0] = log_prob
    out_ref[1] = jnp.where(low, pltpu.roll(first, rows, 1), second)
    out_ref[2] = jnp.broadcast_to(jnp.sum(log_prob, keepdims=True) * (1.0 / (CHIPS * 2 * rows)), log_prob.shape)


def solution(mesh):
    def local_step(hidden, target, norm_gain, head_weight):
        rows, depth = hidden.shape
        vocab = head_weight.shape[1]
        width = pl.cdiv(vocab, 128) * 128
        half = rows // HALVES
        dma = pltpu.SemaphoreType.DMA
        out = pl.pallas_call(
            kernel,
            name="head",
            out_shape=pltpu.VMEM((3, CHIPS, 2 * rows), jnp.float32),
            in_specs=[pl.BlockSpec(memory_space=pl.ANY)] * 4,
            out_specs=pl.BlockSpec(memory_space=pltpu.VMEM),
            scratch_shapes=[
                pltpu.VMEM((rows, depth), jnp.bfloat16),
                pltpu.VMEM((depth,), jnp.bfloat16),
                pltpu.VMEM((CHIPS, 2 * rows), jnp.int32),
                pltpu.VMEM((GROUPS, 6, half, depth), jnp.bfloat16),
                pltpu.VMEM((depth, 2 * width), jnp.bfloat16),
                pltpu.VMEM((STAGES, 128, depth), jnp.bfloat16),
                pltpu.VMEM((vocab % 128, depth), jnp.bfloat16),
                pltpu.VMEM((6 * half, 2 * width), jnp.float32),
                pltpu.VMEM((6 * half, 2 * width), jnp.float32),
                pltpu.VMEM((GROUPS, 6, half, 128), jnp.float32),
                pltpu.VMEM((12, half, 128), jnp.float32),
                pltpu.VMEM((CHIPS, 2, 128), jnp.float32),
                pltpu.VMEM((CHIPS, 2, 128), jnp.float32),
                pltpu.VMEM((1, 128), jnp.float32),
                pltpu.VMEM((2 * CHIPS, 1, 128), jnp.float32),
                dma((EVENTS,)), dma((EVENTS,)), dma((STAGES,)), dma, dma, dma, dma, dma, dma, dma,
                dma((HALVES + 2,)),
            ],
            compiler_params=pltpu.CompilerParams(
                collective_id=0,
                has_side_effects=True,
                vmem_limit_bytes=66_000_000,
            ),
        )(hidden, norm_gain, target.reshape(CHIPS, 2 * rows), head_weight.T)
        return out[0].reshape(-1), out[1].reshape(-1), out[2, 0, 0:1]

    return jax.shard_map(local_step, mesh=mesh, in_specs=(P(("dp", "vp"), None), P("dp"), P(None), P(None, "vp")), out_specs=(P("dp"), P("dp"), P("dp")), check_vma=False)
```

```python
import functools
import itertools

import jax
import jax.numpy as jnp
from jax import lax
from jax.experimental import pallas as pl
from jax.experimental.pallas import tpu as pltpu
from jax.sharding import PartitionSpec as P

NORM_EPS = 1e-6
MESH = pl.DeviceIdType.MESH
SIDE = 4
CHIPS = SIDE**3
OWN = CHIPS - 1
LOW = -3.0e38
DIRS = ((1, 0, 0), (0, 1, 0), (0, 0, 1), (-1, 0, 0), (0, -1, 0), (0, 0, -1))
FULL = 10

PARENT = (
    63, 63, 63, 63, 63, 63, 4, 0, 4, 3, 4, 0, 2, 3, 3, 4, 5, 5, 7, 2, 6, 5, 9, 1, 11, 17, 12, 16, 11, 16, 10, 19,
    9, 8, 16, 7, 26, 12, 14, 19, 15, 13, 35, 18, 30, 29, 28, 35, 28, 36, 31, 31, 26, 41, 46, 41, 43, 39, 32, 46, 52, 49, 51,
)
HALVES = 2
EVENTS = HALVES * (FULL + 1)
GROUPS = EVENTS
AHEAD = 4
STAGES = 4
WIDE = 512


def offsets():
    out = {OWN: (0, 0, 0)}
    for j, parent in enumerate(PARENT):
        out[j] = tuple((a + b) % SIDE for a, b in zip(out[parent], DIRS[j % 6]))
    return out


OFFSET = offsets()
FARTHEST = (SIDE // 2,) * 3


def pieces_of(slot):
    return range(6 * slot, min(6 * slot + 6, OWN))


def place(piece, c):
    if piece == OWN:
        return GROUPS - 1, c
    if piece >= 6 * FULL:
        return HALVES * FULL, piece - 6 * FULL + 3 * c
    return HALVES * (piece // 6) + c, piece % 6


def kernel(hidden_hbm, gain_hbm, target_hbm, head_ref, out_ref, hidden_ref, gain_ref, target_ref, x_ref, w_ref, stage_ref, rest_ref, za_ref, zb_ref,
           tgt_ref, pack_ref, mine_ref, stat_ref, res_ref, fin_ref, send_sem, recv_sem, stage_sem, rest_sem, w_send, w_recv,
           stat_send, stat_recv, fin_send, fin_recv, in_sem):
    rows, depth = hidden_ref.shape
    half = rows // HALVES
    vocab = head_ref.shape[0]
    tiles = pl.cdiv(vocab, 128)
    width = tiles * 128
    me = lax.axis_index("vp")
    group = lax.axis_index("dp")
    core = lax.rem(me, 2)
    chip = me // 2
    coords = (lax.rem(chip, SIDE), lax.rem(chip // SIDE, SIDE), chip // (SIDE * SIDE))
    sign = 1 - 2 * core
    partner = me + sign

    def device(there):
        return (group, there)

    def chip_at(offset):
        c = [lax.rem(coords[i] + sign * offset[i] + 2 * SIDE, SIDE) for i in range(3)]
        return (c[2] * SIDE + c[1]) * SIDE + c[0]

    neighbours = [chip_at(d) * 2 + core for d in DIRS]

    def behind(piece):
        return chip_at([-o for o in OFFSET[piece]])

    def merger(piece):
        return chip_at([SIDE // 2 - o for o in OFFSET[piece]])

    barrier = pltpu.get_barrier_semaphore()
    for there in (*neighbours, partner):
        pl.semaphore_signal(barrier, inc=1, device_id=device(there), device_id_type=MESH)

    def stage_copy(n):
        return pltpu.make_async_copy(head_ref.at[128 * n : 128 * n + 128], stage_ref.at[n % STAGES], stage_sem.at[n % STAGES])

    whole = vocab // 128
    gain_copy = pltpu.make_async_copy(gain_hbm, gain_ref, in_sem.at[HALVES])
    target_copy = pltpu.make_async_copy(target_hbm, target_ref, in_sem.at[HALVES + 1])
    hidden_copies = [
        pltpu.make_async_copy(hidden_hbm.at[c * half : (c + 1) * half], hidden_ref.at[c * half : (c + 1) * half], in_sem.at[c])
        for c in range(HALVES)
    ]
    for copy in (gain_copy, *hidden_copies):
        copy.start()

    def send_event(event):
        c = event % HALVES
        for piece in pieces_of(event // HALVES):
            pltpu.make_async_remote_copy(
                src_ref=x_ref.at[place(PARENT[piece], c)],
                dst_ref=x_ref.at[place(piece, c)],
                send_sem=send_sem.at[event],
                recv_sem=recv_sem.at[event],
                device_id=device(neighbours[piece % 6]),
                device_id_type=MESH,
            ).start()

    def wait_event(event, sem):
        ps = pieces_of(event // HALVES)
        g, d = place(ps.start, event % HALVES)
        block = x_ref.at[g, d : d + len(ps)]
        pltpu.make_async_copy(block, block, sem.at[event]).wait()

    gain_copy.wait()
    gain = gain_ref[...].astype(jnp.float32)
    for c in range(HALVES):
        hidden_copies[c].wait()
        if c == HALVES - 1:
            target_copy.start()
            for n in range(STAGES):
                stage_copy(n).start()
            rest_copy = pltpu.make_async_copy(head_ref.at[128 * whole : vocab], rest_ref, rest_sem)
            rest_copy.start()
        h = hidden_ref[c * half : (c + 1) * half].astype(jnp.float32)
        inv_rms = lax.rsqrt(jnp.mean(h * h, axis=-1, keepdims=True) + NORM_EPS)
        x_ref[GROUPS - 1, c] = (h * inv_rms * gain).astype(jnp.bfloat16)
        if c == 0:
            pl.semaphore_wait(barrier, 7)
        send_event(c)

    def head_copy(n):
        return pltpu.make_async_remote_copy(
            src_ref=w_ref.at[:, 128 * n : 128 * n + 128],
            dst_ref=w_ref.at[:, width + 128 * n : width + 128 * n + 128],
            send_sem=w_send,
            recv_sem=w_recv,
            device_id=device(partner),
            device_id_type=MESH,
        )

    for n in range(tiles):
        if n < whole:
            stage_copy(n).wait()
        else:
            rest_copy.wait()
            stage_ref[n % STAGES, 0 : vocab - 128 * whole] = rest_ref[...]

        def turn(k, carry, n=n):
            for u in range(4):
                at = pl.multiple_of((4 * k + u) * 128, 128)
                w_ref[pl.ds(at, 128), 128 * n : 128 * n + 128] = stage_ref[n % STAGES, :, pl.ds(at, 128)].T
            return carry

        lax.fori_loop(0, depth // 512, turn, 0)
        if n + STAGES < whole:
            stage_copy(n + STAGES).start()
        if n:
            head_copy(n - 1).start()

    lane_ids = lax.broadcasted_iota(jnp.int32, (half, 128), 1)
    row_ids = lax.broadcasted_iota(jnp.int32, (half, 128), 0)
    lanes = lane_ids.astype(jnp.float32)
    last_ok = lane_ids < vocab - (tiles - 1) * 128

    def targets(piece):
        row = target_ref[pl.ds(behind(piece), 1), :].astype(jnp.float32)
        for c in range(HALVES):
            hit = lane_ids == row_ids + (core * rows + c * half)
            column = jnp.sum(jnp.where(hit, row, 0.0), axis=1, keepdims=True)
            tgt_ref[place(piece, c)] = column - lanes

    target_copy.wait()
    for piece in range(CHIPS):
        targets(piece)
        if piece == 0:
            head_copy(tiles - 1).start()

    def comm(event):
        wait_event(event, recv_sem)
        if event < HALVES:
            send_event(event + HALVES)
        if event + AHEAD < EVENTS:
            send_event(event + AHEAD)

    comm(0)
    comm(1)
    partner_head = w_ref.at[:, width : 2 * width]
    pltpu.make_async_copy(partner_head, partner_head, w_recv).wait()

    base = [(me * vocab).astype(jnp.float32), (partner * vocab).astype(jnp.float32)]

    def lane_stats(z_ref, g, d, sides):
        def tile(b, k):
            return z_ref[d * half : (d + 1) * half, (b * tiles + k) * 128 : (b * tiles + k + 1) * 128]

        def masked(k, v, other):
            return jnp.where(last_ok, v, other) if k == tiles - 1 else v

        top = tile(sides[0], 0)
        for b in sides:
            for k in range(tiles):
                top = jnp.maximum(top, masked(k, tile(b, k), LOW))
        total = jnp.zeros_like(top)
        moment = jnp.zeros_like(top)
        picked = jnp.zeros_like(top)
        for b in sides:
            where = tgt_ref[g, d] - base[b]
            for k in range(tiles):
                z = tile(b, k)
                shifted = z - top
                e = jnp.exp(shifted)
                total += masked(k, e, 0.0)
                moment += masked(k, e * shifted, 0.0)
                hit = where == float(128 * k)
                if k == tiles - 1:
                    hit = hit & last_ok
                picked = jnp.where(hit, z, picked)
        return top, total, moment, picked

    def row_stats(stats, pack_at):
        highest = functools.reduce(jnp.maximum, [top for top, _, _, _ in stats])
        row_top = jnp.max(highest, axis=1, keepdims=True)
        totals, moments, picks = [], [], []
        for top, total, moment, picked in stats:
            drop = top - row_top
            scale = jnp.exp(drop)
            totals.append(total * scale)
            moments.append((moment + total * drop) * scale)
            picks.append(picked)
        row_total, row_moment, row_picked = (jnp.sum(functools.reduce(jnp.add, v), axis=1, keepdims=True) for v in (totals, moments, picks))
        pack_ref[pack_at] = jnp.where(lane_ids == 0, row_top, jnp.where(lane_ids == 1, row_total, jnp.where(lane_ids == 2, row_moment, row_picked)))

    def strip_stats(z_ref, g, d, pack_at):
        row_stats([lane_stats(z_ref, g, d, (0, 1))], pack_at)

    def part(g, z_ref, before, other_ref, pack_at):
        x = x_ref[g].reshape(6 * half, depth)
        for n in range(2 * width // WIDE):
            at = slice(n * WIDE, (n + 1) * WIDE)
            for d in range(2 * n, min(2 * n + 2, 6)):
                strip_stats(other_ref, before, d, pack_at(d))
            z_ref[:, at] = jnp.dot(x, w_ref[:, at], preferred_element_type=jnp.float32)

    low = lax.broadcasted_iota(jnp.int32, (1, 128), 1) < rows

    def flush(pieces, first=0):
        for i in range(0, len(pieces), 2):
            block = pack_ref[first + 2 * i : first + 2 * i + 4].reshape(2 * rows, 128).T
            turned = pltpu.roll(block[0:8, :], rows, 1)
            for j, piece in enumerate(pieces[i : i + 2]):
                left, right = (block, turned) if j == 0 else (turned, block)
                mine_ref[piece, 0:1] = jnp.where(low, left[0:1, :], right[1:2, :])
                mine_ref[piece, 1:2] = jnp.where(low, left[2:3, :], right[3:4, :])

    def stat_copy(piece):
        return pltpu.make_async_remote_copy(
            src_ref=mine_ref.at[piece],
            dst_ref=stat_ref.at[piece],
            send_sem=stat_send,
            recv_sem=stat_recv,
            device_id=device(merger(piece) * 2 + core),
            device_id_type=MESH,
        )

    def send_stats(pieces):
        for piece in pieces:
            if OFFSET[piece] == FARTHEST:
                stat_ref[piece] = mine_ref[piece]
            else:
                stat_copy(piece).start()

    def at_turn(turn, first, last, what):
        for t in range(first, last):
            pl.when(turn == t)(functools.partial(what, t))

    def step(turn, carry):
        def before_first(t):
            comm(2 * t - 1)

        def before_second(t):
            comm(2 * t)
            if t == FULL - 2:
                send_stats([*range(18), OWN])
            if t == FULL - 1:
                send_stats(range(18, 42))

        at_turn(turn, 2, FULL, before_first)
        first = jnp.where(turn == 0, GROUPS - 1, 2 * turn - 1)
        part(first, za_ref, jnp.maximum(2 * turn - 2, 0), zb_ref, lambda d: 2 * d)
        at_turn(turn, 1, FULL, before_second)
        part(2 * turn, zb_ref, first, za_ref, lambda d: jnp.where(turn == 0, d, 2 * d + 1))

        @pl.when(turn > 0)
        def _():
            flush([6 * (turn - 1) + i for i in range(6)])

        @pl.when(turn == 0)
        def _():
            flush([OWN])

        return carry

    lax.fori_loop(0, FULL, step, 0)

    comm(2 * FULL - 1)
    part(2 * FULL - 1, za_ref, 2 * FULL - 2, zb_ref, lambda d: 2 * d)
    for d in range(6):
        strip_stats(za_ref, 2 * FULL - 1, d, 2 * d + 1)
    flush(pieces_of(FULL - 1))
    send_stats(range(6 * FULL - 18, 6 * FULL))
    comm(2 * FULL)
    comm(2 * FULL + 1)

    end = 2 * FULL
    away = [p for p in pieces_of(FULL) if OFFSET[p] != FARTHEST]
    here = [p for p in pieces_of(FULL) if OFFSET[p] == FARTHEST]
    strips = [(place(p, c)[1], 2 * i + c) for i, p in enumerate(away + here) for c in range(HALVES)]
    x = x_ref[end].reshape(6 * half, depth)
    zb_ref[:, 0:width] = jnp.dot(x, w_ref[:, 0:width], preferred_element_type=jnp.float32)
    firsts = [lane_stats(zb_ref, end, d, (0,)) for d, _ in strips]
    zb_ref[:, width : 2 * width] = jnp.dot(x, w_ref[:, width : 2 * width], preferred_element_type=jnp.float32)
    for stats, (d, pack_at) in zip(firsts, strips, strict=True):
        row_stats([stats, lane_stats(zb_ref, end, d, (1,))], pack_at)
        if pack_at == 2 * len(away) - 1:
            flush(away)
            send_stats(away)
    flush(here, 2 * len(away))
    send_stats(here)

    arrived = stat_ref.at[0 : CHIPS - 1]
    pltpu.make_async_copy(arrived, arrived, stat_recv).wait()
    tops, moments = stat_ref[:, 0, :], stat_ref[:, 1, :]
    totals, picks = pltpu.roll(tops, rows, 1), pltpu.roll(moments, rows, 1)
    top = jnp.max(tops, axis=0, keepdims=True)
    drop = tops - top
    scale = jnp.exp(drop)
    total = jnp.sum(totals * scale, axis=0, keepdims=True)
    moment = jnp.sum((moments + totals * drop) * scale, axis=0, keepdims=True)
    picked = jnp.sum(picks, axis=0, keepdims=True)
    log_total = jnp.log(total)
    res_ref[...] = jnp.where(low, picked - top - log_total, pltpu.roll(log_total - moment / total, rows, 1))

    origin = core * CHIPS + merger(OWN)
    fin_ref[origin] = res_ref[...]
    steps = [[lax.rem(coords[i] + k, SIDE) for k in range(SIDE)] for i in range(3)]

    def hops(offset):
        return sum(min(o, SIDE - o) for o in offset)

    for x, y, z in sorted(itertools.product(range(SIDE), repeat=3), key=hops, reverse=True):
        there = ((steps[2][z] * SIDE + steps[1][y]) * SIDE + steps[0][x]) * 2
        for side in range(2):
            if hops((x, y, z)) == 0 and side == 1:
                continue
            pltpu.make_async_remote_copy(
                src_ref=res_ref,
                dst_ref=fin_ref.at[origin],
                send_sem=fin_send,
                recv_sem=fin_recv,
                device_id=device(partner if hops((x, y, z)) == 0 else there + side),
                device_id_type=MESH,
            ).start()
    others = fin_ref.at[0 : 2 * CHIPS - 1]
    pltpu.make_async_copy(partner_head, partner_head, w_send).wait()
    for event in range(EVENTS):
        wait_event(event, send_sem)
    pltpu.make_async_copy(arrived, arrived, stat_send).wait()
    pltpu.make_async_copy(others, others, fin_send).wait()

    pltpu.make_async_copy(others, others, fin_recv).wait()
    first, second = fin_ref[0:CHIPS, 0, :], fin_ref[CHIPS:, 0, :]
    log_prob = jnp.where(low, first, pltpu.roll(second, rows, 1))
    out_ref[0] = log_prob
    out_ref[1] = jnp.where(low, pltpu.roll(first, rows, 1), second)
    out_ref[2] = jnp.broadcast_to(jnp.sum(log_prob, keepdims=True) * (1.0 / (CHIPS * 2 * rows)), log_prob.shape)


def solution(mesh):
    def local_step(hidden, target, norm_gain, head_weight):
        rows, depth = hidden.shape
        vocab = head_weight.shape[1]
        width = pl.cdiv(vocab, 128) * 128
        half = rows // HALVES
        dma = pltpu.SemaphoreType.DMA
        out = pl.pallas_call(
            kernel,
            name="head",
            out_shape=pltpu.VMEM((3, CHIPS, 2 * rows), jnp.float32),
            in_specs=[pl.BlockSpec(memory_space=pl.ANY)] * 4,
            out_specs=pl.BlockSpec(memory_space=pltpu.VMEM),
            scratch_shapes=[
                pltpu.VMEM((rows, depth), jnp.bfloat16),
                pltpu.VMEM((depth,), jnp.bfloat16),
                pltpu.VMEM((CHIPS, 2 * rows), jnp.int32),
                pltpu.VMEM((GROUPS, 6, half, depth), jnp.bfloat16),
                pltpu.VMEM((depth, 2 * width), jnp.bfloat16),
                pltpu.VMEM((STAGES, 128, depth), jnp.bfloat16),
                pltpu.VMEM((vocab % 128, depth), jnp.bfloat16),
                pltpu.VMEM((6 * half, 2 * width), jnp.float32),
                pltpu.VMEM((6 * half, 2 * width), jnp.float32),
                pltpu.VMEM((GROUPS, 6, half, 128), jnp.float32),
                pltpu.VMEM((12, half, 128), jnp.float32),
                pltpu.VMEM((CHIPS, 2, 128), jnp.float32),
                pltpu.VMEM((CHIPS, 2, 128), jnp.float32),
                pltpu.VMEM((1, 128), jnp.float32),
                pltpu.VMEM((2 * CHIPS, 1, 128), jnp.float32),
                dma((EVENTS,)), dma((EVENTS,)), dma((STAGES,)), dma, dma, dma, dma, dma, dma, dma,
                dma((HALVES + 2,)),
            ],
            compiler_params=pltpu.CompilerParams(
                collective_id=0,
                has_side_effects=True,
                vmem_limit_bytes=66_000_000,
            ),
        )(hidden, norm_gain, target.reshape(CHIPS, 2 * rows), head_weight.T)
        return out[0].reshape(-1), out[1].reshape(-1), out[2, 0, 0:1]

    return jax.shard_map(local_step, mesh=mesh, in_specs=(P(("dp", "vp"), None), P("dp"), P(None), P(None, "vp")), out_specs=(P("dp"), P("dp"), P("dp")), check_vma=False)
```

```python
import functools
import itertools

import jax
import jax.numpy as jnp
from jax import lax
from jax.experimental import pallas as pl
from jax.experimental.pallas import tpu as pltpu
from jax.sharding import PartitionSpec as P

NORM_EPS = 1e-6
MESH = pl.DeviceIdType.MESH
SIDE = 4
CHIPS = SIDE**3
OWN = CHIPS - 1
LOW = -3.0e38
DIRS = ((1, 0, 0), (0, 1, 0), (0, 0, 1), (-1, 0, 0), (0, -1, 0), (0, 0, -1))
FULL = 10

PARENT = (
    63, 63, 63, 63, 63, 63, 4, 0, 4, 3, 4, 0, 2, 3, 3, 4, 5, 5, 7, 2, 6, 5, 9, 1, 11, 17, 12, 16, 11, 16, 10, 19,
    9, 8, 16, 7, 26, 12, 14, 19, 15, 13, 35, 18, 30, 29, 28, 35, 28, 36, 31, 31, 26, 41, 46, 41, 43, 39, 32, 46, 52, 49, 51,
)
HALVES = 2
EVENTS = HALVES * (FULL + 1)
GROUPS = EVENTS
AHEAD = 4
STAGES = 4
WIDE = 512


def offsets():
    out = {OWN: (0, 0, 0)}
    for j, parent in enumerate(PARENT):
        out[j] = tuple((a + b) % SIDE for a, b in zip(out[parent], DIRS[j % 6]))
    return out


OFFSET = offsets()
FARTHEST = (SIDE // 2,) * 3


def pieces_of(slot):
    return range(6 * slot, min(6 * slot + 6, OWN))


def place(piece, c):
    if piece == OWN:
        return GROUPS - 1, c
    if piece >= 6 * FULL:
        return HALVES * FULL, piece - 6 * FULL + 3 * c
    return HALVES * (piece // 6) + c, piece % 6


def kernel(hidden_hbm, gain_hbm, target_hbm, head_ref, out_ref, hidden_ref, gain_ref, target_ref, x_ref, w_ref, stage_ref, rest_ref, za_ref, zb_ref,
           tgt_ref, pack_ref, mine_ref, stat_ref, res_ref, fin_ref, send_sem, recv_sem, stage_sem, rest_sem, w_send, w_recv,
           stat_send, stat_recv, fin_send, fin_recv, in_sem):
    rows, depth = hidden_ref.shape
    half = rows // HALVES
    vocab = head_ref.shape[0]
    tiles = pl.cdiv(vocab, 128)
    width = tiles * 128
    me = lax.axis_index("vp")
    group = lax.axis_index("dp")
    core = lax.rem(me, 2)
    chip = me // 2
    coords = (lax.rem(chip, SIDE), lax.rem(chip // SIDE, SIDE), chip // (SIDE * SIDE))
    sign = 1 - 2 * core
    partner = me + sign

    def device(there):
        return (group, there)

    def chip_at(offset):
        c = [lax.rem(coords[i] + sign * offset[i] + 2 * SIDE, SIDE) for i in range(3)]
        return (c[2] * SIDE + c[1]) * SIDE + c[0]

    neighbours = [chip_at(d) * 2 + core for d in DIRS]

    def behind(piece):
        return chip_at([-o for o in OFFSET[piece]])

    def merger(piece):
        return chip_at([SIDE // 2 - o for o in OFFSET[piece]])

    barrier = pltpu.get_barrier_semaphore()
    for there in (*neighbours, partner):
        pl.semaphore_signal(barrier, inc=1, device_id=device(there), device_id_type=MESH)

    def stage_copy(n):
        return pltpu.make_async_copy(head_ref.at[128 * n : 128 * n + 128], stage_ref.at[n % STAGES], stage_sem.at[n % STAGES])

    whole = vocab // 128
    gain_copy = pltpu.make_async_copy(gain_hbm, gain_ref, in_sem.at[HALVES])
    target_copy = pltpu.make_async_copy(target_hbm, target_ref, in_sem.at[HALVES + 1])
    hidden_copies = [
        pltpu.make_async_copy(hidden_hbm.at[c * half : (c + 1) * half], hidden_ref.at[c * half : (c + 1) * half], in_sem.at[c])
        for c in range(HALVES)
    ]
    for copy in (gain_copy, *hidden_copies):
        copy.start()

    def send_event(event):
        c = event % HALVES
        for piece in pieces_of(event // HALVES):
            pltpu.make_async_remote_copy(
                src_ref=x_ref.at[place(PARENT[piece], c)],
                dst_ref=x_ref.at[place(piece, c)],
                send_sem=send_sem.at[event],
                recv_sem=recv_sem.at[event],
                device_id=device(neighbours[piece % 6]),
                device_id_type=MESH,
            ).start()

    def wait_event(event, sem):
        ps = pieces_of(event // HALVES)
        g, d = place(ps.start, event % HALVES)
        block = x_ref.at[g, d : d + len(ps)]
        pltpu.make_async_copy(block, block, sem.at[event]).wait()

    gain_copy.wait()
    gain = gain_ref[...].astype(jnp.float32)
    for c in range(HALVES):
        hidden_copies[c].wait()
        if c == HALVES - 1:
            target_copy.start()
            for n in range(STAGES):
                stage_copy(n).start()
            rest_copy = pltpu.make_async_copy(head_ref.at[128 * whole : vocab], rest_ref, rest_sem)
            rest_copy.start()
        h = hidden_ref[c * half : (c + 1) * half].astype(jnp.float32)
        inv_rms = lax.rsqrt(jnp.mean(h * h, axis=-1, keepdims=True) + NORM_EPS)
        x_ref[GROUPS - 1, c] = (h * inv_rms * gain).astype(jnp.bfloat16)
        if c == 0:
            pl.semaphore_wait(barrier, 7)
        send_event(c)

    def head_copy(n):
        return pltpu.make_async_remote_copy(
            src_ref=w_ref.at[:, 128 * n : 128 * n + 128],
            dst_ref=w_ref.at[:, width + 128 * n : width + 128 * n + 128],
            send_sem=w_send,
            recv_sem=w_recv,
            device_id=device(partner),
            device_id_type=MESH,
        )

    for n in range(tiles):
        if n < whole:
            stage_copy(n).wait()
        else:
            rest_copy.wait()
            stage_ref[n % STAGES, 0 : vocab - 128 * whole] = rest_ref[...]

        def turn(k, carry, n=n):
            for u in range(4):
                at = pl.multiple_of((4 * k + u) * 128, 128)
                w_ref[pl.ds(at, 128), 128 * n : 128 * n + 128] = stage_ref[n % STAGES, :, pl.ds(at, 128)].T
            return carry

        lax.fori_loop(0, depth // 512, turn, 0)
        if n + STAGES < whole:
            stage_copy(n + STAGES).start()
        if n:
            head_copy(n - 1).start()

    lane_ids = lax.broadcasted_iota(jnp.int32, (half, 128), 1)
    row_ids = lax.broadcasted_iota(jnp.int32, (half, 128), 0)
    lanes = lane_ids.astype(jnp.float32)
    last_ok = lane_ids < vocab - (tiles - 1) * 128

    def targets(piece):
        row = target_ref[pl.ds(behind(piece), 1), :].astype(jnp.float32)
        for c in range(HALVES):
            hit = lane_ids == row_ids + (core * rows + c * half)
            column = jnp.sum(jnp.where(hit, row, 0.0), axis=1, keepdims=True)
            tgt_ref[place(piece, c)] = column - lanes

    target_copy.wait()
    for piece in range(CHIPS):
        targets(piece)
        if piece == 0:
            head_copy(tiles - 1).start()

    def comm(event):
        wait_event(event, recv_sem)
        if event < HALVES:
            send_event(event + HALVES)
        if event + AHEAD < EVENTS:
            send_event(event + AHEAD)

    comm(0)
    comm(1)
    partner_head = w_ref.at[:, width : 2 * width]
    pltpu.make_async_copy(partner_head, partner_head, w_recv).wait()

    base = [(me * vocab).astype(jnp.float32), (partner * vocab).astype(jnp.float32)]

    def lane_stats(z_ref, at, g, d, sides):
        def tile(b, k):
            return z_ref[at * half : (at + 1) * half, (b * tiles + k) * 128 : (b * tiles + k + 1) * 128]

        def masked(k, v, other):
            return jnp.where(last_ok, v, other) if k == tiles - 1 else v

        top = tile(sides[0], 0)
        for b in sides:
            for k in range(tiles):
                top = jnp.maximum(top, masked(k, tile(b, k), LOW))
        total = jnp.zeros_like(top)
        moment = jnp.zeros_like(top)
        picked = jnp.zeros_like(top)
        for b in sides:
            where = tgt_ref[g, d] - base[b]
            for k in range(tiles):
                z = tile(b, k)
                shifted = z - top
                e = jnp.exp(shifted)
                total += masked(k, e, 0.0)
                moment += masked(k, e * shifted, 0.0)
                hit = where == float(128 * k)
                if k == tiles - 1:
                    hit = hit & last_ok
                picked = jnp.where(hit, z, picked)
        return top, total, moment, picked

    def row_stats(stats, pack_at):
        highest = functools.reduce(jnp.maximum, [top for top, _, _, _ in stats])
        row_top = jnp.max(highest, axis=1, keepdims=True)
        totals, moments, picks = [], [], []
        for top, total, moment, picked in stats:
            drop = top - row_top
            scale = jnp.exp(drop)
            totals.append(total * scale)
            moments.append((moment + total * drop) * scale)
            picks.append(picked)
        row_total, row_moment, row_picked = (jnp.sum(functools.reduce(jnp.add, v), axis=1, keepdims=True) for v in (totals, moments, picks))
        pack_ref[pack_at] = jnp.where(lane_ids == 0, row_top, jnp.where(lane_ids == 1, row_total, jnp.where(lane_ids == 2, row_moment, row_picked)))

    def strip_stats(z_ref, g, d, pack_at):
        row_stats([lane_stats(z_ref, d, g, d, (0, 1))], pack_at)

    def part(g, z_ref, before, other_ref, pack_at):
        x = x_ref[g].reshape(6 * half, depth)
        for n in range(2 * width // WIDE):
            at = slice(n * WIDE, (n + 1) * WIDE)
            for d in range(2 * n, min(2 * n + 2, 6)):
                strip_stats(other_ref, before, d, pack_at(d))
            z_ref[:, at] = jnp.dot(x, w_ref[:, at], preferred_element_type=jnp.float32)

    low = lax.broadcasted_iota(jnp.int32, (1, 128), 1) < rows

    def flush(pieces, first=0):
        for i in range(0, len(pieces), 2):
            block = pack_ref[first + 2 * i : first + 2 * i + 4].reshape(2 * rows, 128).T
            turned = pltpu.roll(block[0:8, :], rows, 1)
            for j, piece in enumerate(pieces[i : i + 2]):
                left, right = (block, turned) if j == 0 else (turned, block)
                mine_ref[piece, 0:1] = jnp.where(low, left[0:1, :], right[1:2, :])
                mine_ref[piece, 1:2] = jnp.where(low, left[2:3, :], right[3:4, :])

    def stat_copy(piece):
        return pltpu.make_async_remote_copy(
            src_ref=mine_ref.at[piece],
            dst_ref=stat_ref.at[piece],
            send_sem=stat_send,
            recv_sem=stat_recv,
            device_id=device(merger(piece) * 2 + core),
            device_id_type=MESH,
        )

    def send_stats(pieces):
        for piece in pieces:
            if OFFSET[piece] == FARTHEST:
                stat_ref[piece] = mine_ref[piece]
            else:
                stat_copy(piece).start()

    def at_turn(turn, first, last, what):
        for t in range(first, last):
            pl.when(turn == t)(functools.partial(what, t))

    def step(turn, carry):
        def before_first(t):
            comm(2 * t - 1)

        def before_second(t):
            comm(2 * t)
            if t == FULL - 2:
                send_stats([*range(18), OWN])
            if t == FULL - 1:
                send_stats(range(18, 42))

        at_turn(turn, 2, FULL, before_first)
        first = jnp.where(turn == 0, GROUPS - 1, 2 * turn - 1)
        part(first, za_ref, jnp.maximum(2 * turn - 2, 0), zb_ref, lambda d: 2 * d)
        at_turn(turn, 1, FULL, before_second)
        part(2 * turn, zb_ref, first, za_ref, lambda d: jnp.where(turn == 0, d, 2 * d + 1))

        @pl.when(turn > 0)
        def _():
            flush([6 * (turn - 1) + i for i in range(6)])

        @pl.when(turn == 0)
        def _():
            flush([OWN])

        return carry

    lax.fori_loop(0, FULL, step, 0)

    comm(2 * FULL - 1)
    part(2 * FULL - 1, za_ref, 2 * FULL - 2, zb_ref, lambda d: 2 * d)
    for d in range(6):
        strip_stats(za_ref, 2 * FULL - 1, d, 2 * d + 1)
    flush(pieces_of(FULL - 1))
    send_stats(range(6 * FULL - 18, 6 * FULL))
    comm(2 * FULL)
    comm(2 * FULL + 1)

    end = 2 * FULL

    def finish(pieces, first):
        strips = [place(p, c)[1] for p in pieces for c in range(HALVES)]
        x = jnp.concatenate([x_ref[end, d] for d in strips], axis=0)
        at = slice(first * half, (first + len(strips)) * half)
        firsts = []
        for b in range(2):
            side = slice(b * width, (b + 1) * width)
            zb_ref[at, side] = jnp.dot(x, w_ref[:, side], preferred_element_type=jnp.float32)
            if b == 0:
                firsts = [lane_stats(zb_ref, first + i, end, d, (0,)) for i, d in enumerate(strips)]
        for i, d in enumerate(strips):
            row_stats([firsts[i], lane_stats(zb_ref, first + i, end, d, (1,))], first + i)
        flush(pieces, first)
        send_stats(pieces)

    away = [p for p in pieces_of(FULL) if OFFSET[p] != FARTHEST]
    here = [p for p in pieces_of(FULL) if OFFSET[p] == FARTHEST]
    finish(away, 0)
    finish(here, HALVES * len(away))

    arrived = stat_ref.at[0 : CHIPS - 1]
    pltpu.make_async_copy(arrived, arrived, stat_recv).wait()
    tops, moments = stat_ref[:, 0, :], stat_ref[:, 1, :]
    totals, picks = pltpu.roll(tops, rows, 1), pltpu.roll(moments, rows, 1)
    top = jnp.max(tops, axis=0, keepdims=True)
    drop = tops - top
    scale = jnp.exp(drop)
    total = jnp.sum(totals * scale, axis=0, keepdims=True)
    moment = jnp.sum((moments + totals * drop) * scale, axis=0, keepdims=True)
    picked = jnp.sum(picks, axis=0, keepdims=True)
    log_total = jnp.log(total)
    res_ref[...] = jnp.where(low, picked - top - log_total, pltpu.roll(log_total - moment / total, rows, 1))

    origin = core * CHIPS + merger(OWN)
    fin_ref[origin] = res_ref[...]
    steps = [[lax.rem(coords[i] + k, SIDE) for k in range(SIDE)] for i in range(3)]

    def hops(offset):
        return sum(min(o, SIDE - o) for o in offset)

    for x, y, z in sorted(itertools.product(range(SIDE), repeat=3), key=hops, reverse=True):
        there = ((steps[2][z] * SIDE + steps[1][y]) * SIDE + steps[0][x]) * 2
        for side in range(2):
            if hops((x, y, z)) == 0 and side == 1:
                continue
            pltpu.make_async_remote_copy(
                src_ref=res_ref,
                dst_ref=fin_ref.at[origin],
                send_sem=fin_send,
                recv_sem=fin_recv,
                device_id=device(partner if hops((x, y, z)) == 0 else there + side),
                device_id_type=MESH,
            ).start()
    others = fin_ref.at[0 : 2 * CHIPS - 1]
    pltpu.make_async_copy(partner_head, partner_head, w_send).wait()
    for event in range(EVENTS):
        wait_event(event, send_sem)
    pltpu.make_async_copy(arrived, arrived, stat_send).wait()
    pltpu.make_async_copy(others, others, fin_send).wait()

    pltpu.make_async_copy(others, others, fin_recv).wait()
    first, second = fin_ref[0:CHIPS, 0, :], fin_ref[CHIPS:, 0, :]
    log_prob = jnp.where(low, first, pltpu.roll(second, rows, 1))
    out_ref[0] = log_prob
    out_ref[1] = jnp.where(low, pltpu.roll(first, rows, 1), second)
    out_ref[2] = jnp.broadcast_to(jnp.sum(log_prob, keepdims=True) * (1.0 / (CHIPS * 2 * rows)), log_prob.shape)


def solution(mesh):
    def local_step(hidden, target, norm_gain, head_weight):
        rows, depth = hidden.shape
        vocab = head_weight.shape[1]
        width = pl.cdiv(vocab, 128) * 128
        half = rows // HALVES
        dma = pltpu.SemaphoreType.DMA
        out = pl.pallas_call(
            kernel,
            name="head",
            out_shape=pltpu.VMEM((3, CHIPS, 2 * rows), jnp.float32),
            in_specs=[pl.BlockSpec(memory_space=pl.ANY)] * 4,
            out_specs=pl.BlockSpec(memory_space=pltpu.VMEM),
            scratch_shapes=[
                pltpu.VMEM((rows, depth), jnp.bfloat16),
                pltpu.VMEM((depth,), jnp.bfloat16),
                pltpu.VMEM((CHIPS, 2 * rows), jnp.int32),
                pltpu.VMEM((GROUPS, 6, half, depth), jnp.bfloat16),
                pltpu.VMEM((depth, 2 * width), jnp.bfloat16),
                pltpu.VMEM((STAGES, 128, depth), jnp.bfloat16),
                pltpu.VMEM((vocab % 128, depth), jnp.bfloat16),
                pltpu.VMEM((6 * half, 2 * width), jnp.float32),
                pltpu.VMEM((6 * half, 2 * width), jnp.float32),
                pltpu.VMEM((GROUPS, 6, half, 128), jnp.float32),
                pltpu.VMEM((12, half, 128), jnp.float32),
                pltpu.VMEM((CHIPS, 2, 128), jnp.float32),
                pltpu.VMEM((CHIPS, 2, 128), jnp.float32),
                pltpu.VMEM((1, 128), jnp.float32),
                pltpu.VMEM((2 * CHIPS, 1, 128), jnp.float32),
                dma((EVENTS,)), dma((EVENTS,)), dma((STAGES,)), dma, dma, dma, dma, dma, dma, dma,
                dma((HALVES + 2,)),
            ],
            compiler_params=pltpu.CompilerParams(
                collective_id=0,
                has_side_effects=True,
                vmem_limit_bytes=66_000_000,
            ),
        )(hidden, norm_gain, target.reshape(CHIPS, 2 * rows), head_weight.T)
        return out[0].reshape(-1), out[1].reshape(-1), out[2, 0, 0:1]

    return jax.shard_map(local_step, mesh=mesh, in_specs=(P(("dp", "vp"), None), P("dp"), P(None), P(None, "vp")), out_specs=(P("dp"), P("dp"), P("dp")), check_vma=False)
```

```python
import functools
import itertools

import jax
import jax.numpy as jnp
from jax import lax
from jax.experimental import pallas as pl
from jax.experimental.pallas import tpu as pltpu
from jax.sharding import PartitionSpec as P

NORM_EPS = 1e-6
MESH = pl.DeviceIdType.MESH
SIDE = 4
CHIPS = SIDE**3
OWN = CHIPS - 1
LOW = -3.0e38
DIRS = ((1, 0, 0), (0, 1, 0), (0, 0, 1), (-1, 0, 0), (0, -1, 0), (0, 0, -1))
FULL = 10

PARENT = (
    63, 63, 63, 63, 63, 63, 4, 0, 4, 3, 4, 0, 2, 3, 3, 4, 5, 5, 7, 2, 6, 5, 9, 1, 11, 17, 12, 16, 11, 16, 10, 19,
    9, 8, 16, 7, 26, 12, 14, 19, 15, 13, 35, 18, 30, 29, 28, 35, 28, 36, 31, 31, 26, 41, 46, 41, 43, 39, 32, 46, 52, 49, 51,
)
HALVES = 2
EVENTS = HALVES * (FULL + 1)
GROUPS = EVENTS
AHEAD = 4
STAGES = 4
WIDE = 512


def offsets():
    out = {OWN: (0, 0, 0)}
    for j, parent in enumerate(PARENT):
        out[j] = tuple((a + b) % SIDE for a, b in zip(out[parent], DIRS[j % 6]))
    return out


OFFSET = offsets()
FARTHEST = (SIDE // 2,) * 3


def pieces_of(slot):
    return range(6 * slot, min(6 * slot + 6, OWN))


def place(piece, c):
    if piece == OWN:
        return GROUPS - 1, c
    if piece >= 6 * FULL:
        return HALVES * FULL, piece - 6 * FULL + 3 * c
    return HALVES * (piece // 6) + c, piece % 6


def kernel(hidden_hbm, gain_hbm, target_hbm, head_ref, out_ref, hidden_ref, gain_ref, target_ref, x_ref, w_ref, stage_ref, rest_ref, za_ref, zb_ref,
           tgt_ref, pack_ref, mine_ref, stat_ref, res_ref, fin_ref, send_sem, recv_sem, stage_sem, rest_sem, w_send, w_recv,
           stat_send, stat_recv, fin_send, fin_recv, in_sem):
    rows, depth = hidden_ref.shape
    half = rows // HALVES
    vocab = head_ref.shape[0]
    tiles = pl.cdiv(vocab, 128)
    width = tiles * 128
    me = lax.axis_index("vp")
    group = lax.axis_index("dp")
    core = lax.rem(me, 2)
    chip = me // 2
    coords = (lax.rem(chip, SIDE), lax.rem(chip // SIDE, SIDE), chip // (SIDE * SIDE))
    sign = 1 - 2 * core
    partner = me + sign

    def device(there):
        return (group, there)

    def chip_at(offset):
        c = [lax.rem(coords[i] + sign * offset[i] + 2 * SIDE, SIDE) for i in range(3)]
        return (c[2] * SIDE + c[1]) * SIDE + c[0]

    neighbours = [chip_at(d) * 2 + core for d in DIRS]

    def behind(piece):
        return chip_at([-o for o in OFFSET[piece]])

    def merger(piece):
        return chip_at([SIDE // 2 - o for o in OFFSET[piece]])

    barrier = pltpu.get_barrier_semaphore()
    for there in (*neighbours, partner):
        pl.semaphore_signal(barrier, inc=1, device_id=device(there), device_id_type=MESH)

    def stage_copy(n):
        return pltpu.make_async_copy(head_ref.at[128 * n : 128 * n + 128], stage_ref.at[n % STAGES], stage_sem.at[n % STAGES])

    whole = vocab // 128
    gain_copy = pltpu.make_async_copy(gain_hbm, gain_ref, in_sem.at[HALVES])
    target_copy = pltpu.make_async_copy(target_hbm, target_ref, in_sem.at[HALVES + 1])
    hidden_copies = [
        pltpu.make_async_copy(hidden_hbm.at[c * half : (c + 1) * half], hidden_ref.at[c * half : (c + 1) * half], in_sem.at[c])
        for c in range(HALVES)
    ]
    for copy in (gain_copy, *hidden_copies):
        copy.start()

    def send_event(event):
        c = event % HALVES
        for piece in pieces_of(event // HALVES):
            pltpu.make_async_remote_copy(
                src_ref=x_ref.at[place(PARENT[piece], c)],
                dst_ref=x_ref.at[place(piece, c)],
                send_sem=send_sem.at[event],
                recv_sem=recv_sem.at[event],
                device_id=device(neighbours[piece % 6]),
                device_id_type=MESH,
            ).start()

    def wait_event(event, sem):
        ps = pieces_of(event // HALVES)
        g, d = place(ps.start, event % HALVES)
        block = x_ref.at[g, d : d + len(ps)]
        pltpu.make_async_copy(block, block, sem.at[event]).wait()

    gain_copy.wait()
    gain = gain_ref[...].astype(jnp.float32)
    for c in range(HALVES):
        hidden_copies[c].wait()
        if c == HALVES - 1:
            target_copy.start()
            for n in range(STAGES):
                stage_copy(n).start()
            rest_copy = pltpu.make_async_copy(head_ref.at[128 * whole : vocab], rest_ref, rest_sem)
            rest_copy.start()
        h = hidden_ref[c * half : (c + 1) * half].astype(jnp.float32)
        inv_rms = lax.rsqrt(jnp.mean(h * h, axis=-1, keepdims=True) + NORM_EPS)
        x_ref[GROUPS - 1, c] = (h * inv_rms * gain).astype(jnp.bfloat16)
        if c == 0:
            pl.semaphore_wait(barrier, 7)
        send_event(c)

    def head_copy(n):
        return pltpu.make_async_remote_copy(
            src_ref=w_ref.at[:, 128 * n : 128 * n + 128],
            dst_ref=w_ref.at[:, width + 128 * n : width + 128 * n + 128],
            send_sem=w_send,
            recv_sem=w_recv,
            device_id=device(partner),
            device_id_type=MESH,
        )

    for n in range(tiles):
        if n < whole:
            stage_copy(n).wait()
        else:
            rest_copy.wait()
            stage_ref[n % STAGES, 0 : vocab - 128 * whole] = rest_ref[...]

        def turn(k, carry, n=n):
            for u in range(4):
                at = pl.multiple_of((4 * k + u) * 128, 128)
                w_ref[pl.ds(at, 128), 128 * n : 128 * n + 128] = stage_ref[n % STAGES, :, pl.ds(at, 128)].T
            return carry

        lax.fori_loop(0, depth // 512, turn, 0)
        if n + STAGES < whole:
            stage_copy(n + STAGES).start()
        if n:
            head_copy(n - 1).start()

    lane_ids = lax.broadcasted_iota(jnp.int32, (half, 128), 1)
    row_ids = lax.broadcasted_iota(jnp.int32, (half, 128), 0)
    lanes = lane_ids.astype(jnp.float32)
    last_ok = lane_ids < vocab - (tiles - 1) * 128

    def targets(piece):
        row = target_ref[pl.ds(behind(piece), 1), :].astype(jnp.float32)
        for c in range(HALVES):
            hit = lane_ids == row_ids + (core * rows + c * half)
            column = jnp.sum(jnp.where(hit, row, 0.0), axis=1, keepdims=True)
            tgt_ref[place(piece, c)] = column - lanes

    target_copy.wait()
    for piece in range(CHIPS):
        targets(piece)
        if piece == 0:
            head_copy(tiles - 1).start()

    def comm(event):
        wait_event(event, recv_sem)
        if event < HALVES:
            send_event(event + HALVES)
        if event + AHEAD < EVENTS:
            send_event(event + AHEAD)

    comm(0)
    comm(1)
    partner_head = w_ref.at[:, width : 2 * width]
    pltpu.make_async_copy(partner_head, partner_head, w_recv).wait()

    base = [(me * vocab).astype(jnp.float32), (partner * vocab).astype(jnp.float32)]

    def lane_stats(z_ref, at, g, d, sides):
        def tile(b, k):
            return z_ref[at * half : (at + 1) * half, (b * tiles + k) * 128 : (b * tiles + k + 1) * 128]

        def masked(k, v, other):
            return jnp.where(last_ok, v, other) if k == tiles - 1 else v

        top = tile(sides[0], 0)
        for b in sides:
            for k in range(tiles):
                top = jnp.maximum(top, masked(k, tile(b, k), LOW))
        total = jnp.zeros_like(top)
        moment = jnp.zeros_like(top)
        picked = jnp.zeros_like(top)
        for b in sides:
            where = tgt_ref[g, d] - base[b]
            for k in range(tiles):
                z = tile(b, k)
                shifted = z - top
                e = jnp.exp(shifted)
                total += masked(k, e, 0.0)
                moment += masked(k, e * shifted, 0.0)
                hit = where == float(128 * k)
                if k == tiles - 1:
                    hit = hit & last_ok
                picked = jnp.where(hit, z, picked)
        return top, total, moment, picked

    def row_stats(stats, pack_at):
        highest = functools.reduce(jnp.maximum, [top for top, _, _, _ in stats])
        row_top = jnp.max(highest, axis=1, keepdims=True)
        totals, moments, picks = [], [], []
        for top, total, moment, picked in stats:
            drop = top - row_top
            scale = jnp.exp(drop)
            totals.append(total * scale)
            moments.append((moment + total * drop) * scale)
            picks.append(picked)
        row_total, row_moment, row_picked = (jnp.sum(functools.reduce(jnp.add, v), axis=1, keepdims=True) for v in (totals, moments, picks))
        pack_ref[pack_at] = jnp.where(lane_ids == 0, row_top, jnp.where(lane_ids == 1, row_total, jnp.where(lane_ids == 2, row_moment, row_picked)))

    def strip_stats(z_ref, g, d, pack_at):
        row_stats([lane_stats(z_ref, d, g, d, (0, 1))], pack_at)

    def part(g, z_ref, before, other_ref, pack_at):
        x = x_ref[g].reshape(6 * half, depth)
        for n in range(2 * width // WIDE):
            at = slice(n * WIDE, (n + 1) * WIDE)
            for d in range(2 * n, min(2 * n + 2, 6)):
                strip_stats(other_ref, before, d, pack_at(d))
            z_ref[:, at] = jnp.dot(x, w_ref[:, at], preferred_element_type=jnp.float32)

    low = lax.broadcasted_iota(jnp.int32, (1, 128), 1) < rows

    def flush(pieces, first=0):
        for i in range(0, len(pieces), 2):
            block = pack_ref[first + 2 * i : first + 2 * i + 4].reshape(2 * rows, 128).T
            turned = pltpu.roll(block[0:8, :], rows, 1)
            for j, piece in enumerate(pieces[i : i + 2]):
                left, right = (block, turned) if j == 0 else (turned, block)
                mine_ref[piece, 0:1] = jnp.where(low, left[0:1, :], right[1:2, :])
                mine_ref[piece, 1:2] = jnp.where(low, left[2:3, :], right[3:4, :])

    def stat_copy(piece):
        return pltpu.make_async_remote_copy(
            src_ref=mine_ref.at[piece],
            dst_ref=stat_ref.at[piece],
            send_sem=stat_send,
            recv_sem=stat_recv,
            device_id=device(merger(piece) * 2 + core),
            device_id_type=MESH,
        )

    def send_stats(pieces):
        for piece in pieces:
            if OFFSET[piece] == FARTHEST:
                stat_ref[piece] = mine_ref[piece]
            else:
                stat_copy(piece).start()

    def at_turn(turn, first, last, what):
        for t in range(first, last):
            pl.when(turn == t)(functools.partial(what, t))

    def step(turn, carry):
        def before_first(t):
            comm(2 * t - 1)

        def before_second(t):
            comm(2 * t)
            if t == FULL - 2:
                send_stats([*range(18), OWN])
            if t == FULL - 1:
                send_stats(range(18, 42))

        at_turn(turn, 2, FULL, before_first)
        first = jnp.where(turn == 0, GROUPS - 1, 2 * turn - 1)
        part(first, za_ref, jnp.maximum(2 * turn - 2, 0), zb_ref, lambda d: 2 * d)
        at_turn(turn, 1, FULL, before_second)
        part(2 * turn, zb_ref, first, za_ref, lambda d: jnp.where(turn == 0, d, 2 * d + 1))

        @pl.when(turn > 0)
        def _():
            flush([6 * (turn - 1) + i for i in range(6)])

        @pl.when(turn == 0)
        def _():
            flush([OWN])

        return carry

    lax.fori_loop(0, FULL, step, 0)

    send_stats(range(6 * FULL - 18, 6 * FULL - 6))
    comm(2 * FULL - 1)
    part(2 * FULL - 1, za_ref, 2 * FULL - 2, zb_ref, lambda d: 2 * d)
    for d in range(6):
        strip_stats(za_ref, 2 * FULL - 1, d, 2 * d + 1)
    flush(pieces_of(FULL - 1))
    send_stats(pieces_of(FULL - 1))
    comm(2 * FULL)
    comm(2 * FULL + 1)

    end = 2 * FULL

    def finish(pieces, first):
        strips = [place(p, c)[1] for p in pieces for c in range(HALVES)]
        x = jnp.concatenate([x_ref[end, d] for d in strips], axis=0)
        at = slice(first * half, (first + len(strips)) * half)
        firsts = []
        for b in range(2):
            side = slice(b * width, (b + 1) * width)
            zb_ref[at, side] = jnp.dot(x, w_ref[:, side], preferred_element_type=jnp.float32)
            if b == 0:
                firsts = [lane_stats(zb_ref, first + i, end, d, (0,)) for i, d in enumerate(strips)]
        for i, d in enumerate(strips):
            row_stats([firsts[i], lane_stats(zb_ref, first + i, end, d, (1,))], first + i)
        flush(pieces, first)
        send_stats(pieces)

    away = [p for p in pieces_of(FULL) if OFFSET[p] != FARTHEST]
    here = [p for p in pieces_of(FULL) if OFFSET[p] == FARTHEST]
    finish(away, 0)
    finish(here, HALVES * len(away))

    arrived = stat_ref.at[0 : CHIPS - 1]
    pltpu.make_async_copy(arrived, arrived, stat_recv).wait()
    tops, moments = stat_ref[:, 0, :], stat_ref[:, 1, :]
    totals, picks = pltpu.roll(tops, rows, 1), pltpu.roll(moments, rows, 1)
    top = jnp.max(tops, axis=0, keepdims=True)
    drop = tops - top
    scale = jnp.exp(drop)
    total = jnp.sum(totals * scale, axis=0, keepdims=True)
    moment = jnp.sum((moments + totals * drop) * scale, axis=0, keepdims=True)
    picked = jnp.sum(picks, axis=0, keepdims=True)
    log_total = jnp.log(total)
    res_ref[...] = jnp.where(low, picked - top - log_total, pltpu.roll(log_total - moment / total, rows, 1))

    origin = core * CHIPS + merger(OWN)
    fin_ref[origin] = res_ref[...]
    steps = [[lax.rem(coords[i] + k, SIDE) for k in range(SIDE)] for i in range(3)]

    def hops(offset):
        return sum(min(o, SIDE - o) for o in offset)

    for x, y, z in sorted(itertools.product(range(SIDE), repeat=3), key=hops, reverse=True):
        there = ((steps[2][z] * SIDE + steps[1][y]) * SIDE + steps[0][x]) * 2
        for side in range(2):
            if hops((x, y, z)) == 0 and side == 1:
                continue
            pltpu.make_async_remote_copy(
                src_ref=res_ref,
                dst_ref=fin_ref.at[origin],
                send_sem=fin_send,
                recv_sem=fin_recv,
                device_id=device(partner if hops((x, y, z)) == 0 else there + side),
                device_id_type=MESH,
            ).start()
    others = fin_ref.at[0 : 2 * CHIPS - 1]
    pltpu.make_async_copy(partner_head, partner_head, w_send).wait()
    for event in range(EVENTS):
        wait_event(event, send_sem)
    pltpu.make_async_copy(arrived, arrived, stat_send).wait()
    pltpu.make_async_copy(others, others, fin_send).wait()

    pltpu.make_async_copy(others, others, fin_recv).wait()
    first, second = fin_ref[0:CHIPS, 0, :], fin_ref[CHIPS:, 0, :]
    log_prob = jnp.where(low, first, pltpu.roll(second, rows, 1))
    out_ref[0] = log_prob
    out_ref[1] = jnp.where(low, pltpu.roll(first, rows, 1), second)
    out_ref[2] = jnp.broadcast_to(jnp.sum(log_prob, keepdims=True) * (1.0 / (CHIPS * 2 * rows)), log_prob.shape)


def solution(mesh):
    def local_step(hidden, target, norm_gain, head_weight):
        rows, depth = hidden.shape
        vocab = head_weight.shape[1]
        width = pl.cdiv(vocab, 128) * 128
        half = rows // HALVES
        dma = pltpu.SemaphoreType.DMA
        out = pl.pallas_call(
            kernel,
            name="head",
            out_shape=pltpu.VMEM((3, CHIPS, 2 * rows), jnp.float32),
            in_specs=[pl.BlockSpec(memory_space=pl.ANY)] * 4,
            out_specs=pl.BlockSpec(memory_space=pltpu.VMEM),
            scratch_shapes=[
                pltpu.VMEM((rows, depth), jnp.bfloat16),
                pltpu.VMEM((depth,), jnp.bfloat16),
                pltpu.VMEM((CHIPS, 2 * rows), jnp.int32),
                pltpu.VMEM((GROUPS, 6, half, depth), jnp.bfloat16),
                pltpu.VMEM((depth, 2 * width), jnp.bfloat16),
                pltpu.VMEM((STAGES, 128, depth), jnp.bfloat16),
                pltpu.VMEM((vocab % 128, depth), jnp.bfloat16),
                pltpu.VMEM((6 * half, 2 * width), jnp.float32),
                pltpu.VMEM((6 * half, 2 * width), jnp.float32),
                pltpu.VMEM((GROUPS, 6, half, 128), jnp.float32),
                pltpu.VMEM((12, half, 128), jnp.float32),
                pltpu.VMEM((CHIPS, 2, 128), jnp.float32),
                pltpu.VMEM((CHIPS, 2, 128), jnp.float32),
                pltpu.VMEM((1, 128), jnp.float32),
                pltpu.VMEM((2 * CHIPS, 1, 128), jnp.float32),
                dma((EVENTS,)), dma((EVENTS,)), dma((STAGES,)), dma, dma, dma, dma, dma, dma, dma,
                dma((HALVES + 2,)),
            ],
            compiler_params=pltpu.CompilerParams(
                collective_id=0,
                has_side_effects=True,
                vmem_limit_bytes=66_000_000,
            ),
        )(hidden, norm_gain, target.reshape(CHIPS, 2 * rows), head_weight.T)
        return out[0].reshape(-1), out[1].reshape(-1), out[2, 0, 0:1]

    return jax.shard_map(local_step, mesh=mesh, in_specs=(P(("dp", "vp"), None), P("dp"), P(None), P(None, "vp")), out_specs=(P("dp"), P("dp"), P("dp")), check_vma=False)
```
